32 devices in a mesh: prow: 8 (over z, x), pcol: 4 (over y, core).
Axes of the slice: x: 2, y: 2, z: 4, core: 2. Of those that a mesh axis runs over, the one named last changes fastest.
Arguments:
- a_matrix: bfloat16 [32768, 512], P('prow', 'pcol'), may hold values from -6 to 6
- l_panel: bfloat16 [32768, 256], P('prow', 'pcol'), may hold values from -0.375 to 0.375
- l_inverse: bfloat16 [256, 256], replicated, may hold values from -1 to 1
- pivots: int32 [256], replicated, may hold values from 0 to 32767, as said below
Outputs:
- updated: bfloat16 [32768, 512], P('prow', 'pcol')
The draws below stay inside these ranges and needn't reach their ends.
Inputs may be any that keep to these rules, and one draw needn't show every extreme that they name: pivots[j] >= j for every j.
All inputs are finite; a program needn't handle non-finite values.
Results may differ from the reference program's by a relative error of at most 0.0039.
Values may be sent and summed in bfloat16 or wider, within the bound.
A program may use at most 64 MiB of HBM per device.

```python
import math
import jax
import jax.numpy as jnp
from jax import lax

N = 32768
NB = 256
ROWS_DEV = 4096
WIDTH = 512
N_PROW = 8


def draw_l_inverse(key, part):
    sub_key = jax.random.fold_in(key, 11)
    spread_scale = 0.6 / math.sqrt(NB)
    entries = jnp.clip(jax.random.normal(sub_key, (NB, NB), jnp.float32), -4.0, 4.0) * spread_scale
    triangle = jnp.tril(entries, -1) + jnp.eye(NB, dtype=jnp.float32)
    return triangle.astype(jnp.bfloat16)


def draw_pivots(key, part):
    sub_key = jax.random.fold_in(key, 7)
    starts = jnp.arange(NB, dtype=jnp.int32)
    offsets = jax.random.randint(sub_key, (NB,), 0, N - starts, dtype=jnp.int32)
    chosen = starts + offsets
    chosen = chosen.at[0].set(0)
    return chosen.at[NB - 1].set(N - 1)


def shard_levels(rng, shape, shards, low, high):
    gain, own = 1.0, jax.random.fold_in(rng, 6)
    for position, parts in shards:
        steps = jnp.exp(jax.random.uniform(jax.random.fold_in(own, position), (parts,), jnp.float32, low / len(shards), high / len(shards)))
        gain = gain * jnp.repeat(steps, shape[position] // parts).reshape([-1 if axis == position else 1 for axis in range(len(shape))])
    return gain


def noise(rng, dims, deviation, reach, shards=(), held_as=jnp.bfloat16):
    array = deviation * jax.random.normal(rng, dims, jnp.float32)
    if shards:
        array = array * shard_levels(rng, dims, shards, -0.22, 0.18)
    return jnp.clip(array, -reach, reach).astype(held_as)


def setup_inputs(seed: int = 0) -> dict:
    arg_keys = jax.random.split(jax.random.key(seed), 5)
    return {
        "a_matrix": noise(arg_keys[0], (N, WIDTH), 1.0, 6.0, ((0, 8), (1, 4))),
        "l_panel": noise(arg_keys[1], (N, NB), NB ** -0.5, 0.375, ((0, 8), (1, 4))),
        "l_inverse": draw_l_inverse(jax.random.fold_in(arg_keys[4], 71), 0),
        "pivots": draw_pivots(jax.random.fold_in(arg_keys[4], 71), 0),
    }


def swap_plan(pivots, panel_width):
    slot_ids = jnp.arange(panel_width, dtype=jnp.int32)
    earlier = slot_ids[None, :] < slot_ids[:, None]
    hits = (pivots[None, :] == slot_ids[:, None]) & earlier
    pointer = jnp.max(jnp.where(hits, slot_ids[None, :], -1), axis=1).astype(jnp.int32)
    chain = jnp.where(pointer >= 0, pointer, slot_ids).astype(jnp.int32)
    for _ in range(panel_width.bit_length()):
        chain = jnp.take(chain, chain).astype(jnp.int32)
    same = pivots[None, :] == pivots[:, None]
    previous = jnp.max(jnp.where(same & earlier, slot_ids[None, :], -1), axis=1).astype(jnp.int32)
    top_source = jnp.where(previous >= 0, jnp.take(chain, jnp.maximum(previous, 0)), pivots).astype(jnp.int32)
    later = slot_ids[None, :] > slot_ids[:, None]
    is_last = jnp.logical_not(jnp.any(same & later, axis=1))
    return top_source, chain, is_last


def global_of_stored(stored):
    return ((stored % ROWS_DEV) // NB * N_PROW + stored // ROWS_DEV) * NB + stored % NB


def stored_of_global(global_rows):
    return ((global_rows // NB) % N_PROW) * ROWS_DEV + (global_rows // (NB * N_PROW)) * NB + global_rows % NB


def reference(a_matrix, l_panel, l_inverse, pivots):
    top_source, moved_source, is_last = swap_plan(pivots, NB)
    targets = jnp.where(is_last & (pivots >= NB), pivots, N).astype(jnp.int32)
    row_source = jnp.arange(N, dtype=jnp.int32).at[targets].set(moved_source, mode="drop")
    row_source = row_source.at[:NB].set(top_source)
    stored = jnp.arange(N, dtype=jnp.int32)
    source_stored = stored_of_global(row_source[global_of_stored(stored)]).astype(jnp.int32)
    swapped = jnp.take(a_matrix, source_stored, axis=0)
    top_rows = jnp.take(a_matrix, stored_of_global(top_source).astype(jnp.int32), axis=0)
    u_block = jnp.dot(l_inverse, top_rows, preferred_element_type=jnp.float32).astype(jnp.bfloat16)
    width_total = a_matrix.shape[1]

    def update_block(pair):
        a_rows, l_rows = pair
        product = jnp.dot(l_rows, u_block, preferred_element_type=jnp.float32)
        return (a_rows.astype(jnp.float32) - product).astype(jnp.bfloat16)

    blocks = lax.map(update_block, (swapped.reshape(N_PROW, ROWS_DEV, width_total), l_panel.reshape(N_PROW, ROWS_DEV, NB)))
    updated = blocks.reshape(N, width_total)
    return updated.at[:NB].set(u_block)
```

```python
import functools

import jax
import jax.numpy as jnp
from jax import lax
from jax.experimental import pallas as pl
from jax.experimental.pallas import tpu as pltpu
from jax.sharding import PartitionSpec as P

MESH = pl.DeviceIdType.MESH
F32 = jnp.float32
BF16 = jnp.bfloat16
CORES = 2
LOADS = 4


def one_hot(mask):
    return jnp.where(mask, 1.0, 0.0).astype(BF16)


def column_of(pv_row):
    nb = pv_row.shape[1]
    slot = lax.broadcasted_iota(jnp.int32, (nb, nb), 0)
    other = lax.broadcasted_iota(jnp.int32, (nb, nb), 1)
    return jnp.max(jnp.where(slot == other, pv_row, -1.0), axis=1, keepdims=True)


def swap_plan(pv_row, pv_col):
    nb = pv_row.shape[1]
    slot = lax.broadcasted_iota(jnp.int32, (nb, nb), 0).astype(F32)
    other = lax.broadcasted_iota(jnp.int32, (nb, nb), 1).astype(F32)
    slot_col = lax.broadcasted_iota(jnp.int32, (nb, 1), 0).astype(F32)
    earlier = other < slot
    pointer = jnp.max(jnp.where((pv_row == slot) & earlier, other, -1.0), axis=1, keepdims=True)
    chain = one_hot(other == jnp.where(pointer >= 0, pointer, slot_col))
    for _ in range((nb - 1).bit_length()):
        chain = jnp.dot(chain, chain, preferred_element_type=F32).astype(BF16)
    same = pv_row == pv_col
    previous = jnp.max(jnp.where(same & earlier, other, -1.0), axis=1, keepdims=True)
    via = jnp.dot(one_hot(other == previous), chain, preferred_element_type=F32).astype(BF16)
    repeated = jnp.max(jnp.where(same & (slot > other), 1.0, 0.0), axis=0, keepdims=True)
    landing = jnp.where((repeated < 0.5) & (pv_row >= nb), pv_row, -1.0)
    return previous, via, chain, landing


def kernel(
    n_prow, n_pcol, bounds,
    a_hbm, l_hbm, inv_hbm, pv_hbm, out_v,
    a_v, l_full, inv_v, pv_ref, part, got, mine, tops, origs,
    load_sem, a_sem,
    p1_send, p1_recv, p2_send, p2_recv, o1_send, o1_recv, o2_send, o2_recv, o_here,
    y_send, y_recv, m_send, m_recv, f_send, f_recv,
    owner_up, rest_up, mate_in,
):
    rows, width = a_v.shape
    nb = inv_v.shape[0]
    n_red, piece, _ = part.shape
    n_y = n_pcol // CORES
    chunks = len(bounds) - 1
    me = lax.axis_index("prow")
    col = lax.axis_index("pcol")
    y, core = col // CORES, col % CORES
    mate = y * CORES + (1 - core)

    def y_peer(d):
        return lax.rem(y + d, n_y) * CORES + core

    def y_from(d):
        return lax.rem(y + n_y - d, n_y) * CORES + core

    def to(d):
        return lax.rem(me + d, n_prow)

    def frm(d):
        return lax.rem(me + n_prow - d, n_prow)

    def lower(d):
        return me + d >= n_prow

    def is_red(index):
        return index < n_red

    def if_red(index, fn):
        pl.when(is_red(index))(fn)

    slot = lax.rem(me, n_red)

    barrier = pltpu.get_barrier_semaphore()
    for d in range(1, n_y):
        pl.semaphore_signal(barrier, inc=1, device_id=(me, y_peer(d)), device_id_type=MESH)

    @pl.when(core == 1)
    def _():
        pl.semaphore_signal(barrier, inc=1, device_id=(me, mate), device_id_type=MESH)

    for d in range(1, n_prow):
        @pl.when(is_red(me) & jnp.logical_not(lower(d)))
        def _():
            pl.semaphore_signal(barrier, inc=1, device_id=(to(d), col), device_id_type=MESH)

    pv_load = pltpu.make_async_copy(pv_hbm, pv_ref, load_sem.at[0])
    pv_load.start()
    block = rows // LOADS
    a_loads = [
        pltpu.make_async_copy(
            a_hbm.at[pl.ds(k * block, block)], a_v.at[pl.ds(k * block, block)], a_sem.at[k])
        for k in range(LOADS)
    ]
    for load in a_loads:
        load.start()
    l_load = pltpu.make_async_copy(l_hbm, l_full.at[col], load_sem.at[1])
    inv_load = pltpu.make_async_copy(inv_hbm, inv_v, load_sem.at[2])

    def cols(k):
        return pl.ds(bounds[k], bounds[k + 1] - bounds[k])

    def sent(k, fn):
        if bounds[k + 1] <= nb:
            pl.when(me > 0)(fn)
        else:
            fn()

    y_copies = {}
    for k in range(chunks):
        for d in range(1, n_y):
            y_copies[d, k] = pltpu.make_async_remote_copy(
                l_hbm.at[:, cols(k)], l_full.at[col, :, cols(k)],
                y_send.at[d, k], y_recv.at[d, k], device_id=(me, y_peer(d)), device_id_type=MESH)
    m_copy = pltpu.make_async_remote_copy(
        l_hbm, l_full.at[col], m_send, m_recv, device_id=(me, mate), device_id_type=MESH)

    def enter():
        pl.semaphore_wait(
            barrier, n_y - 1 + jnp.minimum(me, n_red) + jnp.where(core == 0, 1, 0))
        for k in range(chunks):
            for d in range(1, n_y):
                sent(k, y_copies[d, k].start)
        for d in range(1, n_prow):
            @pl.when(is_red(me) & lower(d))
            def _():
                pl.semaphore_signal(owner_up, inc=1, device_id=(to(d), col), device_id_type=MESH)

            @pl.when(jnp.logical_not(is_red(me)) & is_red(to(d)))
            def _():
                pl.semaphore_signal(rest_up, inc=1, device_id=(to(d), col), device_id_type=MESH)

        @pl.when(core == 0)
        def _():
            pl.semaphore_signal(mate_in, inc=1, device_id=(me, mate), device_id_type=MESH)
            m_copy.start()

    pl.when(is_red(me))(enter)
    l_load.start()
    inv_load.start()

    def global_rows(shape, axis, start):
        local = lax.broadcasted_iota(jnp.int32, shape, axis) + start
        return ((local // nb * n_prow + me) * nb + local % nb).astype(F32)

    pv_load.wait()
    pv_row = pv_ref[...].astype(F32)
    pv_col = column_of(pv_row)
    total = jnp.zeros((nb, width), F32)
    for k in range(LOADS):
        a_loads[k].wait()
        pick = one_hot(pv_col == global_rows((1, block), 1, k * block))
        total = total + jnp.dot(pick, a_v[pl.ds(k * block, block), :], preferred_element_type=F32)
    part[...] = total.astype(BF16).reshape(n_red, piece, width)

    pl.when(jnp.logical_not(is_red(me)))(enter)

    p1_copies = {}
    for d in range(1, n_prow):
        t = to(d)
        p1_copies[d] = pltpu.make_async_remote_copy(
            part.at[lax.rem(t, n_red)], got.at[d], p1_send.at[d], p1_recv.at[d],
            device_id=(t, col), device_id_type=MESH)
        pl.when(is_red(t) & lower(d))(p1_copies[d].start)

    @pl.when(me < n_red - 1)
    def _():
        pl.semaphore_wait(owner_up, n_red - 1 - me)

    o1_copies = [
        pltpu.make_async_remote_copy(
            a_v.at[pl.ds(t * piece, piece)], origs.at[t], o1_send.at[t], o1_recv,
            device_id=(t, col), device_id_type=MESH)
        for t in range(1, n_red)
    ]
    o_locals = [
        pltpu.make_async_copy(a_v.at[pl.ds(t * piece, piece)], origs.at[t], o_here.at[t])
        for t in range(n_red)
    ]

    @pl.when(me == 0)
    def _():
        for copy in o_locals:
            copy.start()
        for copy in o1_copies:
            copy.start()

    for d in range(1, n_prow):
        pl.when(is_red(to(d)) & jnp.logical_not(lower(d)))(p1_copies[d].start)

    @pl.when(core == 1)
    def _():
        pl.semaphore_wait(mate_in, 1)
        m_copy.start()

    previous, via, chain, landing = swap_plan(pv_row, pv_col)

    f_copies = {}
    for k in range(chunks):
        for d in range(1, n_y):
            src = y_from(d)
            f_copies[d, k] = pltpu.make_async_remote_copy(
                l_full.at[src, :, cols(k)], l_full.at[src, :, cols(k)],
                f_send.at[d, k], f_recv.at[d, k], device_id=(me, mate), device_id_type=MESH)

    def forward(k):
        if k >= chunks:
            return

        def go():
            for d in range(1, n_y):
                y_copies[d, k].wait_recv()
                f_copies[d, k].start()

        sent(k, go)

    o2_copies, p2_copies = {}, {}
    for d in range(1, n_prow):
        o2_copies[d] = pltpu.make_async_remote_copy(
            origs.at[slot], origs.at[slot], o2_send.at[d], o2_recv.at[d],
            device_id=(to(d), col), device_id_type=MESH)
        p2_copies[d] = pltpu.make_async_remote_copy(
            mine, tops.at[slot], p2_send.at[d], p2_recv.at[d],
            device_id=(to(d), col), device_id_type=MESH)

    def not_first(d, fn):
        pl.when(me + d != n_prow)(fn)

    def send_orig():
        @pl.when(me == 0)
        def _():
            for copy in o_locals:
                copy.wait()

        @pl.when(me > 0)
        def _():
            pltpu.make_async_remote_copy(
                a_v.at[pl.ds(0, piece)], origs.at[slot], o1_send.at[0], o1_recv,
                device_id=(0, col), device_id_type=MESH).wait_recv()

        pl.semaphore_wait(rest_up, n_prow - n_red)
        for d in range(1, n_prow):
            not_first(d, o2_copies[d].start)

    forward(0)
    if_red(me, send_orig)
    forward(1)
    forward(2)

    def reduce_and_send():
        acc = part[slot].astype(F32)
        for d in range(1, n_prow):
            p1_copies[d].wait_recv()
            acc = acc + got[d].astype(F32)
        mine[...] = acc.astype(BF16)
        tops[slot] = acc.astype(BF16)
        for d in range(1, n_prow):
            p2_copies[d].start()

    if_red(me, reduce_and_send)
    forward(3)

    @pl.when(me > 0)
    def _():
        for d in range(1, n_prow):
            if_red(frm(d), o2_copies[d].wait_recv)

    orig = origs[...].reshape(nb, width)
    moved = jnp.dot(chain, orig, preferred_element_type=F32).astype(BF16)
    again = jnp.dot(via, orig, preferred_element_type=F32).astype(BF16)
    moved = jnp.concatenate([moved, jnp.ones((nb, width), BF16)], axis=1)
    step = min(512, rows)
    for start in range(0, rows, step):
        here = one_hot(landing == global_rows((step, 1), 0, start))
        both = jnp.dot(here, moved, preferred_element_type=F32)
        rows_k = pl.ds(start, step)
        out_v[rows_k, :] = jnp.where(
            both[:, width:] > 0.5, both[:, :width], a_v[rows_k, :].astype(F32)).astype(BF16)

    forward(4)
    for d in range(1, n_prow):
        if_red(frm(d), p2_copies[d].wait_recv)
    inv_load.wait()
    top_rows = jnp.where(previous >= 0, again, tops[...].reshape(nb, width))
    u_block = jnp.dot(inv_v[...], top_rows, preferred_element_type=F32).astype(BF16)

    def arrived(k):
        def go():
            for d in range(1, n_y):
                f_copies[d, k].wait_recv()
        sent(k, go)

    def update(first, last):
        for k in range(first, last):
            arrived(k)
        start, stop = bounds[first], bounds[last]
        rows_k = pl.ds(start, stop - start)
        panel = l_full[:, :, rows_k].reshape(nb, stop - start)
        product = lax.dot_general(
            panel, u_block, (((0,), (0,)), ((), ())), preferred_element_type=F32)
        out_v[rows_k, :] = (out_v[rows_k, :].astype(F32) - product).astype(BF16)

    def top_update(k):
        @pl.when(me > 0)
        def _():
            update(k, k + 1)

        @pl.when(me == 0)
        def _():
            rows_k = cols(k)
            out_v[rows_k, :] = u_block[bounds[k]:bounds[k + 1], :]

    top = sum(1 for k in range(chunks) if bounds[k + 1] <= nb)
    m_copy.wait_recv()
    l_load.wait()
    for k in range(5, chunks - 2):
        forward(k)
    for k in range(top):
        top_update(k)
    mid = max(top, chunks - 4)
    if mid > top:
        update(top, mid)
    forward(chunks - 2) if chunks - 2 >= 5 else None
    late = max(mid, chunks - 2)
    if late > mid:
        update(mid, late)
    forward(chunks - 1) if chunks - 1 >= 5 else None
    for k in range(late, chunks):
        update(k, k + 1)

    @pl.when(me == 0)
    def _():
        for copy in o1_copies:
            copy.wait_send()

    m_copy.wait_send()
    for d in range(1, n_prow):
        if_red(to(d), p1_copies[d].wait_send)

    def drain():
        for d in range(1, n_prow):
            not_first(d, o2_copies[d].wait_send)
            p2_copies[d].wait_send()

    if_red(me, drain)
    for d, k in y_copies:
        sent(k, y_copies[d, k].wait_send)
        sent(k, f_copies[d, k].wait_send)


def hbm(array):
    return pltpu.with_memory_space_constraint(array, pltpu.HBM)


def chunk_bounds(rows, nb):
    bounds = [0, nb]
    while bounds[-1] < rows:
        bounds.append(min(bounds[-1] + 2 * nb, rows))
    return tuple(bounds)


def body(n_prow, n_pcol, a_matrix, l_panel, l_inverse, pivots):
    rows, width = a_matrix.shape
    nb = l_inverse.shape[0]
    depth = l_panel.shape[1]
    n_red = min(n_prow // 2, nb // 16)
    piece = nb // n_red
    n_y = n_pcol // CORES
    bounds = chunk_bounds(rows, nb)
    chunks = len(bounds) - 1
    dma = pltpu.SemaphoreType.DMA
    flag = pltpu.SemaphoreType.REGULAR
    return pl.pallas_call(
        functools.partial(kernel, n_prow, n_pcol, bounds),
        out_shape=jax.ShapeDtypeStruct((rows, width), BF16),
        in_specs=[pl.BlockSpec(memory_space=pl.ANY)] * 4,
        out_specs=pl.BlockSpec(memory_space=pltpu.VMEM),
        scratch_shapes=[
            pltpu.VMEM((rows, width), BF16),
            pltpu.VMEM((n_pcol, depth, rows), BF16),
            pltpu.VMEM((nb, nb), BF16),
            pltpu.VMEM((1, nb), jnp.int32),
            pltpu.VMEM((n_red, piece, width), BF16),
            pltpu.VMEM((n_prow, piece, width), BF16),
            pltpu.VMEM((piece, width), BF16),
            pltpu.VMEM((n_red, piece, width), BF16),
            pltpu.VMEM((n_red, piece, width), BF16),
            dma((3,)), dma((LOADS,)),
            dma((n_prow,)), dma((n_prow,)), dma((n_prow,)), dma((n_prow,)),
            dma((n_red,)), dma, dma((n_prow,)), dma((n_prow,)), dma((n_red,)),
            dma((n_y, chunks)), dma((n_y, chunks)), dma, dma,
            dma((n_y, chunks)), dma((n_y, chunks)),
            flag, flag, flag,
        ],
        compiler_params=pltpu.CompilerParams(
            collective_id=0, has_side_effects=True, vmem_limit_bytes=24 * 2 ** 20),
    )(hbm(a_matrix), hbm(l_panel.T), hbm(l_inverse), hbm(pivots.reshape(1, nb)))


def solution(mesh):
    n_prow, n_pcol = mesh.shape["prow"], mesh.shape["pcol"]
    in_specs = (P("prow", "pcol"), P("prow", "pcol"), P(), P())
    return jax.shard_map(
        functools.partial(body, n_prow, n_pcol),
        mesh=mesh, in_specs=in_specs, out_specs=P("prow", "pcol"), check_vma=False)
```

```python
import functools

import jax
import jax.numpy as jnp
from jax import lax
from jax.experimental import pallas as pl
from jax.experimental.pallas import tpu as pltpu
from jax.sharding import PartitionSpec as P

MESH = pl.DeviceIdType.MESH
F32 = jnp.float32
BF16 = jnp.bfloat16
CORES = 2
LOADS = 2
ENTER_AFTER = 0


def one_hot(mask):
    return jnp.where(mask, 1.0, 0.0).astype(BF16)


def column_of(pv_row):
    nb = pv_row.shape[1]
    slot = lax.broadcasted_iota(jnp.int32, (nb, nb), 0)
    other = lax.broadcasted_iota(jnp.int32, (nb, nb), 1)
    return jnp.max(jnp.where(slot == other, pv_row, -1.0), axis=1, keepdims=True)


def swap_plan(pv_row, pv_col):
    nb = pv_row.shape[1]
    slot = lax.broadcasted_iota(jnp.int32, (nb, nb), 0).astype(F32)
    other = lax.broadcasted_iota(jnp.int32, (nb, nb), 1).astype(F32)
    slot_col = lax.broadcasted_iota(jnp.int32, (nb, 1), 0).astype(F32)
    earlier = other < slot
    pointer = jnp.max(jnp.where((pv_row == slot) & earlier, other, -1.0), axis=1, keepdims=True)
    chain = one_hot(other == jnp.where(pointer >= 0, pointer, slot_col))
    for _ in range((nb - 1).bit_length()):
        chain = jnp.dot(chain, chain, preferred_element_type=F32).astype(BF16)
    same = pv_row == pv_col
    previous = jnp.max(jnp.where(same & earlier, other, -1.0), axis=1, keepdims=True)
    via = jnp.dot(one_hot(other == previous), chain, preferred_element_type=F32).astype(BF16)
    repeated = jnp.max(jnp.where(same & (slot > other), 1.0, 0.0), axis=0, keepdims=True)
    landing = jnp.where((repeated < 0.5) & (pv_row >= nb), pv_row, -1.0)
    return previous, via, chain, landing


def kernel(
    n_prow, n_pcol, bounds, tail,
    a_hbm, l_hbm, inv_hbm, pv_hbm, out_v,
    a_v, l_full, inv_v, pv_ref, part, got, mine, tops, origs,
    load_sem, a_sem, send_sem, recv_sem, y_recv, f_recv, flags,
):
    p1_send, p2_send, o1_send, o2_send, y_send, m_send, f_send = (send_sem.at[i] for i in range(7))
    p1_recv, p2_recv, o1_recv, o2_recv, m_recv = (recv_sem.at[i] for i in range(5))
    owner_up, rest_up, mate_in = (flags.at[i] for i in range(3))
    rows, width = a_v.shape
    nb = inv_v.shape[0]
    n_red, piece, _ = part.shape
    depth = l_full.shape[1]
    n_y = n_pcol // CORES
    chunks = len(bounds) - 1
    top = sum(1 for k in range(chunks) if bounds[k + 1] <= nb)
    me = lax.axis_index("prow")
    col = lax.axis_index("pcol")
    y, core = col // CORES, col % CORES
    mate = y * CORES + (1 - core)

    def y_peer(d):
        return lax.rem(y + d, n_y) * CORES + core

    def y_from(d):
        return lax.rem(y + n_y - d, n_y) * CORES + core

    def to(d):
        return lax.rem(me + d, n_prow)

    def frm(d):
        return lax.rem(me + n_prow - d, n_prow)

    def lower(d):
        return me + d >= n_prow

    def is_red(index):
        return index < n_red

    def if_red(index, fn):
        pl.when(is_red(index))(fn)

    slot = lax.rem(me, n_red)

    barrier = pltpu.get_barrier_semaphore()
    for d in range(1, n_y):
        pl.semaphore_signal(barrier, inc=1, device_id=(me, y_peer(d)), device_id_type=MESH)

    @pl.when(core == 1)
    def _():
        pl.semaphore_signal(barrier, inc=1, device_id=(me, mate), device_id_type=MESH)

    for d in range(1, n_prow):
        @pl.when(is_red(me) & jnp.logical_not(lower(d)))
        def _():
            pl.semaphore_signal(barrier, inc=1, device_id=(to(d), y * CORES), device_id_type=MESH)

    pv_load = pltpu.make_async_copy(pv_hbm, pv_ref, load_sem.at[0])
    pv_load.start()
    block = rows // LOADS
    a_loads = [
        pltpu.make_async_copy(
            a_hbm.at[pl.ds(k * block, block)], a_v.at[pl.ds(k * block, block)], a_sem.at[k])
        for k in range(LOADS)
    ]
    for load in a_loads:
        load.start()
    l_load = pltpu.make_async_copy(l_hbm, l_full.at[col], load_sem.at[1])
    inv_load = pltpu.make_async_copy(inv_hbm, inv_v, load_sem.at[0])

    def cols(k):
        return pl.ds(bounds[k], bounds[k + 1] - bounds[k])

    def sent(k, fn):
        if bounds[k + 1] <= nb:
            pl.when(me > 0)(fn)
        else:
            fn()

    def both(chip, k):
        return l_full.at[pl.ds(chip * CORES, CORES), :, cols(k)]

    y_copies = {}
    for k in range(chunks):
        for d in range(1, n_y):
            src, dst = l_hbm.at[:, cols(k)], l_full.at[col, :, cols(k)]
            if k >= tail:
                src = dst = both(y, k)
            y_copies[d, k] = pltpu.make_async_remote_copy(
                src, dst, y_send, y_recv.at[d - 1, k], device_id=(me, y_peer(d)), device_id_type=MESH)
    m_copy = pltpu.make_async_remote_copy(
        l_hbm, l_full.at[col], m_send, m_recv, device_id=(me, mate), device_id_type=MESH)

    def enter():
        pl.semaphore_wait(
            barrier, n_y - 1 + jnp.where(core == 0, 1 + CORES * jnp.minimum(me, n_red), 0))
        for k in range(tail):
            for d in range(1, n_y):
                sent(k, y_copies[d, k].start)
        @pl.when(core == 0)
        def _():
            pl.semaphore_signal(mate_in, inc=1, device_id=(me, mate), device_id_type=MESH)
            m_copy.start()
            for d in range(1, n_prow):
                for c in range(CORES):
                    there = (to(d), y * CORES + c)

                    @pl.when(is_red(me) & lower(d))
                    def _():
                        pl.semaphore_signal(owner_up, inc=1, device_id=there, device_id_type=MESH)

                    @pl.when(jnp.logical_not(is_red(me)) & is_red(to(d)))
                    def _():
                        pl.semaphore_signal(rest_up, inc=1, device_id=there, device_id_type=MESH)

    at_once = (core == 1) | (me == 0)
    pl.when(at_once)(enter)
    l_load.start()

    def global_rows(shape, axis, start):
        local = lax.broadcasted_iota(jnp.int32, shape, axis) + start
        return ((local // nb * n_prow + me) * nb + local % nb).astype(F32)

    pv_load.wait()
    inv_load.start()
    pv_row = pv_ref[...].astype(F32)
    pv_col = column_of(pv_row)
    total = jnp.zeros((nb, width), F32)
    for k in range(LOADS):
        a_loads[k].wait()
        pick = one_hot(pv_col == global_rows((1, block), 1, k * block))
        total = total + jnp.dot(pick, a_v[pl.ds(k * block, block), :], preferred_element_type=F32)
        if k == ENTER_AFTER:
            pl.when(jnp.logical_not(at_once))(enter)
    part[...] = total.astype(BF16).reshape(n_red, piece, width)

    @pl.when(core == 1)
    def _():
        pl.semaphore_wait(mate_in, 1)
        m_copy.start()

    p1_copies = {}
    for d in range(1, n_prow):
        t = to(d)
        p1_copies[d] = pltpu.make_async_remote_copy(
            part.at[lax.rem(t, n_red)], got.at[d], p1_send, p1_recv,
            device_id=(t, col), device_id_type=MESH)
        pl.when(is_red(t) & lower(d))(p1_copies[d].start)

    inv_load.wait()
    pv_row = pv_ref[...].astype(F32)
    previous, via, chain, landing = swap_plan(pv_row, column_of(pv_row))

    @pl.when(me < n_red - 1)
    def _():
        pl.semaphore_wait(owner_up, n_red - 1 - me)

    o1_copies = [
        pltpu.make_async_remote_copy(
            a_v.at[pl.ds(t * piece, piece)], origs.at[pl.ds(t * piece, piece)], o1_send, o1_recv,
            device_id=(t, col), device_id_type=MESH)
        for t in range(1, n_red)
    ]
    o_local = pltpu.make_async_copy(a_v.at[pl.ds(0, nb)], origs, o1_recv)

    @pl.when(me == 0)
    def _():
        o_local.start()
        for copy in o1_copies:
            copy.start()

    for d in range(1, n_prow):
        pl.when(is_red(to(d)) & jnp.logical_not(lower(d)))(p1_copies[d].start)

    m_copy.wait_recv()
    l_load.wait()

    @pl.when(core == 1)
    def _():
        for k in range(tail, chunks):
            for d in range(1, n_y):
                y_copies[d, k].start()

    f_copies = {}
    for k in range(chunks):
        for d in range(1, n_y):
            src = l_full.at[y_from(d), :, cols(k)]
            if k >= tail:
                src = both(y_from(d) // CORES, k)
            f_copies[d, k] = pltpu.make_async_remote_copy(
                src, src, f_send, f_recv.at[d - 1, k], device_id=(me, mate), device_id_type=MESH)

    def forward(k):
        if k >= chunks:
            return

        def go():
            for d in range(1, n_y):
                y_copies[d, k].wait_recv()
                f_copies[d, k].start()

        if k >= tail:
            pl.when(core == 1)(go)
        else:
            sent(k, go)

    own_rows = origs.at[pl.ds(slot * piece, piece)]
    o2_copies, p2_copies = {}, {}
    for d in range(1, n_prow):
        o2_copies[d] = pltpu.make_async_remote_copy(
            own_rows, own_rows, o2_send, o2_recv,
            device_id=(to(d), col), device_id_type=MESH)
        p2_copies[d] = pltpu.make_async_remote_copy(
            mine, tops.at[pl.ds(slot * piece, piece)], p2_send, p2_recv,
            device_id=(to(d), col), device_id_type=MESH)

    def not_first(d, fn):
        pl.when(me + d != n_prow)(fn)

    def send_orig():
        @pl.when(me == 0)
        def _():
            o_local.wait()

        @pl.when(me > 0)
        def _():
            pltpu.make_async_remote_copy(
                a_v.at[pl.ds(0, piece)], own_rows, o1_send, o1_recv,
                device_id=(0, col), device_id_type=MESH).wait_recv()

        pl.semaphore_wait(rest_up, n_prow - n_red)
        for d in range(1, n_prow):
            not_first(d, o2_copies[d].start)

    def arrive(ref, sem):
        pltpu.make_async_copy(ref, ref, sem).wait()

    def gather(ref, sem):
        if_red(me, lambda: arrive(ref.at[pl.ds(0, nb - piece)], sem))
        pl.when(jnp.logical_not(is_red(me)))(lambda: arrive(ref, sem))

    if_red(me, send_orig)
    forward(0)
    forward(1)

    def reduce_and_send():
        acc = part[slot].astype(F32)
        arrive(got.at[pl.ds(1, n_prow - 1)], p1_recv)
        for d in range(1, n_prow):
            acc = acc + got[d].astype(F32)
        mine[...] = acc.astype(BF16)
        tops[pl.ds(slot * piece, piece), :] = acc.astype(BF16)
        for d in range(1, n_prow):
            p2_copies[d].start()

    if_red(me, reduce_and_send)
    forward(2)

    late = [tail - 1] if tail - 1 > 2 else []
    far = (core == 1) | (me >= n_prow * 3 // 4)
    for k in late:
        pl.when(far)(functools.partial(forward, k))

    pl.when(me > 0)(lambda: gather(origs, o2_recv))
    orig = origs[...]
    moved = jnp.dot(chain, orig, preferred_element_type=F32).astype(BF16)
    again = jnp.dot(via, orig, preferred_element_type=F32).astype(BF16)
    moved = jnp.concatenate([moved, jnp.ones((nb, width), BF16)], axis=1)
    step = min(512, rows)
    for start in range(0, rows, step):
        here = one_hot(landing == global_rows((step, 1), 0, start))
        both = jnp.dot(here, moved, preferred_element_type=F32)
        rows_k = pl.ds(start, step)
        out_v[rows_k, :] = jnp.where(
            both[:, width:] > 0.5, both[:, :width], a_v[rows_k, :].astype(F32)).astype(BF16)

    for k in late:
        pl.when(jnp.logical_not(far))(functools.partial(forward, k))
    forward(tail)
    gather(tops, p2_recv)
    top_rows = jnp.where(previous >= 0, again, tops[...])
    u_block = jnp.dot(inv_v[...], top_rows, preferred_element_type=F32).astype(BF16)

    def arrived(k):
        def go():
            for d in range(1, n_y):
                f_copies[d, k].wait_recv()
        if k >= tail:
            pl.when(core == 0)(go)
        else:
            sent(k, go)

    def update(first, last):
        for k in range(first, last):
            arrived(k)
        start, stop = bounds[first], bounds[last]
        rows_k = pl.ds(start, stop - start)
        panel = l_full[:, :, rows_k].reshape(nb, stop - start)
        product = lax.dot_general(
            panel, u_block, (((0,), (0,)), ((), ())), preferred_element_type=F32)
        out_v[rows_k, :] = (out_v[rows_k, :].astype(F32) - product).astype(BF16)

    most = max(top, tail - 1)

    @pl.when(me > 0)
    def _():
        update(0, most)

    @pl.when(me == 0)
    def _():
        out_v[pl.ds(0, bounds[top]), :] = u_block[:bounds[top], :]
        if most > top:
            update(top, most)

    for k in range(tail + 1, chunks):
        forward(k)
    if min(tail + 1, chunks) > most:
        update(most, min(tail + 1, chunks))
    if chunks > tail + 1:
        update(tail + 1, chunks)

    @pl.when(me == 0)
    def _():
        arrive(origs.at[pl.ds(0, nb - piece)], o1_send)

    m_copy.wait_send()
    if_red(me, lambda: arrive(part.at[pl.ds(0, n_red - 1)], p1_send))
    pl.when(jnp.logical_not(is_red(me)))(lambda: arrive(part, p1_send))

    def drain():
        @pl.when(me == 0)
        def _():
            arrive(got.at[pl.ds(1, n_prow - 1)], o2_send)

        @pl.when(me > 0)
        def _():
            arrive(got.at[pl.ds(1, n_prow - 2)], o2_send)

        arrive(got.at[pl.ds(1, n_prow - 1)], p2_send)

    if_red(me, drain)

    def sent_all(lanes):
        tiles = lanes * (n_y - 1) // 128
        if tiles:
            full = rows // 128
            count = next((n for n in range(1, n_pcol + 1) if tiles % n == 0 and tiles // n <= full), 0)
            parts = [(count, tiles // count)] if count else [(tiles // full, full), (1, tiles % full)]
            for count, wide in parts:
                whole = l_full.at[pl.ds(0, count), :, pl.ds(0, wide * 128)]
                arrive(whole, y_send)
                arrive(whole, f_send)

    for skip, here in ((0, me > 0), (bounds[top], me == 0)):
        pl.when(here & (core == 0))(functools.partial(sent_all, bounds[tail] - skip))
        pl.when(here & (core == 1))(functools.partial(sent_all, 2 * rows - bounds[tail] - skip))


def hbm(array):
    return pltpu.with_memory_space_constraint(array, pltpu.HBM)


def chunk_bounds(rows, nb):
    last = min(5 * nb, (rows - nb) // 2)
    bounds = [0, nb]
    while bounds[-1] < rows - last:
        bounds.append(min(bounds[-1] + 4 * nb, rows - last))
    tail = len(bounds) - 1
    if last == 5 * nb:
        bounds += [rows - 5 * nb // 2, rows - nb]
    return (*bounds, rows), tail


def body(n_prow, n_pcol, a_matrix, l_panel, l_inverse, pivots):
    rows, width = a_matrix.shape
    nb = l_inverse.shape[0]
    depth = l_panel.shape[1]
    n_red = min(n_prow // 2, nb // 16)
    piece = nb // n_red
    n_y = n_pcol // CORES
    bounds, tail = chunk_bounds(rows, nb)
    chunks = len(bounds) - 1
    dma = pltpu.SemaphoreType.DMA
    flag = pltpu.SemaphoreType.REGULAR
    return pl.pallas_call(
        functools.partial(kernel, n_prow, n_pcol, bounds, tail),
        out_shape=jax.ShapeDtypeStruct((rows, width), BF16),
        in_specs=[pl.BlockSpec(memory_space=pl.ANY)] * 4,
        out_specs=pl.BlockSpec(memory_space=pltpu.VMEM),
        scratch_shapes=[
            pltpu.VMEM((rows, width), BF16),
            pltpu.VMEM((n_pcol, depth, rows), BF16),
            pltpu.VMEM((nb, nb), BF16),
            pltpu.VMEM((1, nb), jnp.int32),
            pltpu.VMEM((n_red, piece, width), BF16),
            pltpu.VMEM((n_prow, piece, width), BF16),
            pltpu.VMEM((piece, width), BF16),
            pltpu.VMEM((nb, width), BF16),
            pltpu.VMEM((nb, width), BF16),
            dma((2,)), dma((LOADS,)), dma((7,)), dma((5,)),
            dma((max(n_y - 1, 1), chunks)), dma((max(n_y - 1, 1), chunks)), flag((3,)),
        ],
        compiler_params=pltpu.CompilerParams(
            collective_id=0, has_side_effects=True, vmem_limit_bytes=24 * 2 ** 20),
    )(hbm(a_matrix), hbm(l_panel.T), hbm(l_inverse), hbm(pivots.reshape(1, nb)))


def solution(mesh):
    n_prow, n_pcol = mesh.shape["prow"], mesh.shape["pcol"]
    in_specs = (P("prow", "pcol"), P("prow", "pcol"), P(), P())
    return jax.shard_map(
        functools.partial(body, n_prow, n_pcol),
        mesh=mesh, in_specs=in_specs, out_specs=P("prow", "pcol"), check_vma=False)
```

```python
import functools

import jax
import jax.numpy as jnp
from jax import lax
from jax.experimental import pallas as pl
from jax.experimental.pallas import tpu as pltpu
from jax.sharding import PartitionSpec as P

MESH = pl.DeviceIdType.MESH
F32 = jnp.float32
BF16 = jnp.bfloat16
CORES = 2
LOADS = 2
ENTER_AFTER = 0


def one_hot(mask):
    return jnp.where(mask, 1.0, 0.0).astype(BF16)


def column_of(pv_row):
    nb = pv_row.shape[1]
    slot = lax.broadcasted_iota(jnp.int32, (nb, nb), 0)
    other = lax.broadcasted_iota(jnp.int32, (nb, nb), 1)
    return jnp.max(jnp.where(slot == other, pv_row, -1.0), axis=1, keepdims=True)


def swap_plan(pv_row, pv_col):
    nb = pv_row.shape[1]
    slot = lax.broadcasted_iota(jnp.int32, (nb, nb), 0).astype(F32)
    other = lax.broadcasted_iota(jnp.int32, (nb, nb), 1).astype(F32)
    slot_col = lax.broadcasted_iota(jnp.int32, (nb, 1), 0).astype(F32)
    earlier = other < slot
    pointer = jnp.max(jnp.where((pv_row == slot) & earlier, other, -1.0), axis=1, keepdims=True)
    chain = one_hot(other == jnp.where(pointer >= 0, pointer, slot_col))
    for _ in range((nb - 1).bit_length()):
        chain = jnp.dot(chain, chain, preferred_element_type=F32).astype(BF16)
    same = pv_row == pv_col
    previous = jnp.max(jnp.where(same & earlier, other, -1.0), axis=1, keepdims=True)
    via = jnp.dot(one_hot(other == previous), chain, preferred_element_type=F32).astype(BF16)
    repeated = jnp.max(jnp.where(same & (slot > other), 1.0, 0.0), axis=0, keepdims=True)
    landing = jnp.where((repeated < 0.5) & (pv_row >= nb), pv_row, -1.0)
    return previous, via, chain, landing


def kernel(
    n_prow, n_pcol, bounds, tail,
    a_hbm, l_hbm, inv_hbm, pv_hbm, out_v, l_full, u_out,
    a_v, here_v, inv_v, pv_ref, part, got, mine, tops, origs,
    load_sem, a_sem, send_sem, recv_sem, y_recv, f_recv, flags,
):
    p1_send, p2_send, o1_send, o2_send, y_send, m_send, f_send = (send_sem.at[i] for i in range(7))
    p1_recv, p2_recv, o1_recv, o2_recv, m_recv = (recv_sem.at[i] for i in range(5))
    owner_up, rest_up, mate_in = (flags.at[i] for i in range(3))
    rows, width = a_v.shape
    nb = inv_v.shape[0]
    n_red, piece, _ = part.shape
    depth = l_full.shape[1]
    n_y = n_pcol // CORES
    chunks = len(bounds) - 1
    top = sum(1 for k in range(chunks) if bounds[k + 1] <= nb)
    me = lax.axis_index("prow")
    col = lax.axis_index("pcol")
    y, core = col // CORES, col % CORES
    mate = y * CORES + (1 - core)

    def y_peer(d):
        return lax.rem(y + d, n_y) * CORES + core

    def y_from(d):
        return lax.rem(y + n_y - d, n_y) * CORES + core

    def to(d):
        return lax.rem(me + d, n_prow)

    def frm(d):
        return lax.rem(me + n_prow - d, n_prow)

    def lower(d):
        return me + d >= n_prow

    def is_red(index):
        return index < n_red

    def if_red(index, fn):
        pl.when(is_red(index))(fn)

    slot = lax.rem(me, n_red)

    barrier = pltpu.get_barrier_semaphore()
    for d in range(1, n_y):
        pl.semaphore_signal(barrier, inc=1, device_id=(me, y_peer(d)), device_id_type=MESH)

    @pl.when(core == 1)
    def _():
        pl.semaphore_signal(barrier, inc=1, device_id=(me, mate), device_id_type=MESH)

    pv_load = pltpu.make_async_copy(pv_hbm, pv_ref, load_sem.at[0])
    pv_load.start()
    block = rows // LOADS
    a_loads = [
        pltpu.make_async_copy(
            a_hbm.at[pl.ds(k * block, block)], a_v.at[pl.ds(k * block, block)], a_sem.at[k])
        for k in range(LOADS)
    ]
    for load in a_loads:
        load.start()
    for d in range(1, n_prow):
        @pl.when(is_red(me) & jnp.logical_not(lower(d)))
        def _():
            pl.semaphore_signal(barrier, inc=1, device_id=(to(d), y * CORES), device_id_type=MESH)

    l_load = pltpu.make_async_copy(l_hbm, l_full.at[col], load_sem.at[1])
    inv_load = pltpu.make_async_copy(inv_hbm, inv_v, load_sem.at[0])

    def cols(k):
        return pl.ds(bounds[k], bounds[k + 1] - bounds[k])

    def sent(k, fn):
        if bounds[k + 1] <= nb:
            pl.when(me > 0)(fn)
        else:
            fn()

    def both(chip, k):
        return l_full.at[pl.ds(chip * CORES, CORES), :, cols(k)]

    y_copies = {}
    for k in range(chunks):
        for d in range(1, n_y):
            src, dst = l_hbm.at[:, cols(k)], l_full.at[col, :, cols(k)]
            if k >= tail:
                src = dst = both(y, k)
            y_copies[d, k] = pltpu.make_async_remote_copy(
                src, dst, y_send, y_recv.at[d - 1, k], device_id=(me, y_peer(d)), device_id_type=MESH)
    last = chunks - 1
    y_twice = [
        pltpu.make_async_remote_copy(
            both(y, last), both(y, last), y_send, y_recv.at[d - 1, last],
            device_id=(me, y_peer(d) - core), device_id_type=MESH)
        for d in range(1, n_y)
    ]
    m_copy = pltpu.make_async_remote_copy(
        l_hbm, l_full.at[col], m_send, m_recv, device_id=(me, mate), device_id_type=MESH)

    def enter():
        pl.semaphore_wait(
            barrier, n_y - 1 + jnp.where(core == 0, 1 + CORES * jnp.minimum(me, n_red), 0))
        for k in range(tail):
            for d in range(1, n_y):
                sent(k, y_copies[d, k].start)
        @pl.when(core == 0)
        def _():
            pl.semaphore_signal(mate_in, inc=1, device_id=(me, mate), device_id_type=MESH)
            m_copy.start()
            for d in range(1, n_prow):
                for c in range(CORES):
                    there = (to(d), y * CORES + c)

                    @pl.when(is_red(me) & lower(d))
                    def _():
                        pl.semaphore_signal(owner_up, inc=1, device_id=there, device_id_type=MESH)

                    @pl.when(jnp.logical_not(is_red(me)) & is_red(to(d)))
                    def _():
                        pl.semaphore_signal(rest_up, inc=1, device_id=there, device_id_type=MESH)

    at_once = (core == 1) | (me == 0)
    pl.when(at_once)(enter)
    l_load.start()

    def global_rows(shape, axis, start):
        local = lax.broadcasted_iota(jnp.int32, shape, axis) + start
        return ((local // nb * n_prow + me) * nb + local % nb).astype(F32)

    pv_load.wait()
    inv_load.start()
    pv_row = pv_ref[...].astype(F32)
    pv_col = column_of(pv_row)
    total = jnp.zeros((nb, width), F32)
    for k in range(LOADS):
        a_loads[k].wait()
        pick = one_hot(pv_col == global_rows((1, block), 1, k * block))
        total = total + jnp.dot(pick, a_v[pl.ds(k * block, block), :], preferred_element_type=F32)
        if k == ENTER_AFTER:
            pl.when(jnp.logical_not(at_once))(enter)
    part[...] = total.astype(BF16).reshape(n_red, piece, width)

    @pl.when(core == 1)
    def _():
        pl.semaphore_wait(mate_in, 1)
        m_copy.start()

    p1_copies = {}
    for d in range(1, n_prow):
        t = to(d)
        p1_copies[d] = pltpu.make_async_remote_copy(
            part.at[lax.rem(t, n_red)], got.at[d], p1_send, p1_recv,
            device_id=(t, col), device_id_type=MESH)
        pl.when(is_red(t) & lower(d))(p1_copies[d].start)

    inv_load.wait()
    pv_row = pv_ref[...].astype(F32)
    previous, via, chain, landing = swap_plan(pv_row, column_of(pv_row))

    @pl.when(me < n_red - 1)
    def _():
        pl.semaphore_wait(owner_up, n_red - 1 - me)

    o1_copies = [
        pltpu.make_async_remote_copy(
            a_v.at[pl.ds(t * piece, piece)], origs.at[pl.ds(t * piece, piece)], o1_send, o1_recv,
            device_id=(t, col), device_id_type=MESH)
        for t in range(1, n_red)
    ]
    o_local = pltpu.make_async_copy(a_v.at[pl.ds(0, nb)], origs, o1_recv)

    @pl.when(me == 0)
    def _():
        o_local.start()
        for copy in o1_copies:
            copy.start()

    for d in range(1, n_prow):
        pl.when(is_red(to(d)) & jnp.logical_not(lower(d)))(p1_copies[d].start)

    m_copy.wait_recv()
    l_load.wait()

    @pl.when(core == 1)
    def _():
        for k in range(tail, chunks):
            for d in range(1, n_y):
                if k == last:
                    y_twice[d - 1].start()
                y_copies[d, k].start()

    f_copies = {}
    for k in range(chunks):
        for d in range(1, n_y):
            src = l_full.at[y_from(d), :, cols(k)]
            if k >= tail:
                src = both(y_from(d) // CORES, k)
            f_copies[d, k] = pltpu.make_async_remote_copy(
                src, src, f_send, f_recv.at[d - 1, k], device_id=(me, mate), device_id_type=MESH)

    def forward(k):
        if k >= chunks:
            return

        def go():
            for d in range(1, n_y):
                y_copies[d, k].wait_recv()
                f_copies[d, k].start()

        if k == last:
            for d in range(1, n_y):
                y_copies[d, k].wait_recv()
        elif k >= tail:
            pl.when(core == 1)(go)
        else:
            sent(k, go)

    own_rows = origs.at[pl.ds(slot * piece, piece)]
    o2_copies, p2_copies = {}, {}
    for d in range(1, n_prow):
        o2_copies[d] = pltpu.make_async_remote_copy(
            own_rows, own_rows, o2_send, o2_recv,
            device_id=(to(d), col), device_id_type=MESH)
        p2_copies[d] = pltpu.make_async_remote_copy(
            mine, tops.at[pl.ds(slot * piece, piece)], p2_send, p2_recv,
            device_id=(to(d), col), device_id_type=MESH)

    def not_first(d, fn):
        pl.when(me + d != n_prow)(fn)

    def send_orig():
        @pl.when(me == 0)
        def _():
            o_local.wait()

        @pl.when(me > 0)
        def _():
            pltpu.make_async_remote_copy(
                a_v.at[pl.ds(0, piece)], own_rows, o1_send, o1_recv,
                device_id=(0, col), device_id_type=MESH).wait_recv()

        pl.semaphore_wait(rest_up, n_prow - n_red)
        for d in range(1, n_prow):
            not_first(d, o2_copies[d].start)

    def arrive(ref, sem):
        pltpu.make_async_copy(ref, ref, sem).wait()

    def gather(ref, sem):
        if_red(me, lambda: arrive(ref.at[pl.ds(0, nb - piece)], sem))
        pl.when(jnp.logical_not(is_red(me)))(lambda: arrive(ref, sem))

    if_red(me, send_orig)
    step = min(512, rows)
    for start in range(0, rows, step):
        rows_k = pl.ds(start, step)
        here = one_hot(landing == global_rows((step, 1), 0, start))
        here_v[rows_k, :] = here
        hit = jnp.dot(here, jnp.ones((nb, width), BF16), preferred_element_type=F32)
        out_v[rows_k, :] = jnp.where(hit > 0.5, 0.0, a_v[rows_k, :].astype(F32)).astype(BF16)

    forward(0)

    def reduce_and_send():
        acc = part[slot].astype(F32)
        arrive(got.at[pl.ds(1, n_prow - 1)], p1_recv)
        for d in range(1, n_prow):
            acc = acc + got[d].astype(F32)
        mine[...] = acc.astype(BF16)
        tops[pl.ds(slot * piece, piece), :] = acc.astype(BF16)
        for d in range(1, n_prow):
            pl.when(me + d == n_prow)(p2_copies[d].start)
        for d in range(1, n_prow):
            not_first(d, p2_copies[d].start)

    if_red(me, reduce_and_send)
    forward(1)
    forward(2)

    late = [tail - 1] if tail - 1 > 2 else []
    far = (core == 1) | (me >= n_prow * 3 // 4)
    for k in late:
        pl.when(far)(functools.partial(forward, k))

    pl.when(me > 0)(lambda: gather(origs, o2_recv))
    orig = origs[...]
    moved = jnp.dot(chain, orig, preferred_element_type=F32).astype(BF16)
    again = jnp.dot(via, orig, preferred_element_type=F32).astype(BF16)
    for start in range(0, rows, step):
        rows_k = pl.ds(start, step)
        landed = jnp.dot(here_v[rows_k, :], moved, preferred_element_type=F32)
        out_v[rows_k, :] = (out_v[rows_k, :].astype(F32) + landed).astype(BF16)

    for k in late:
        pl.when(jnp.logical_not(far))(functools.partial(forward, k))
    if tail < last:
        forward(tail)
    gather(tops, p2_recv)
    top_rows = jnp.where(previous >= 0, again, tops[...])
    u_block = jnp.dot(inv_v[...], top_rows, preferred_element_type=F32).astype(BF16)

    def arrived(k):
        def go():
            for d in range(1, n_y):
                f_copies[d, k].wait_recv()
        if last > k >= tail:
            pl.when(core == 0)(go)
        elif k < tail:
            sent(k, go)

    def update(first, last):
        for k in range(first, last):
            arrived(k)
        start, stop = bounds[first], bounds[last]
        rows_k = pl.ds(start, stop - start)
        panel = l_full[:, :, rows_k].reshape(nb, stop - start)
        product = lax.dot_general(
            panel, u_block, (((0,), (0,)), ((), ())), preferred_element_type=F32)
        out_v[rows_k, :] = (out_v[rows_k, :].astype(F32) - product).astype(BF16)

    most = max(top, tail - 1)

    @pl.when(me > 0)
    def _():
        update(0, most)

    @pl.when(me == 0)
    def _():
        out_v[pl.ds(0, bounds[top]), :] = u_block[:bounds[top], :]
        if most > top:
            update(top, most)

    u_out[...] = u_block
    for k in range(tail + 1, last):
        forward(k)
    split = min(tail + 1, last)
    if split > most:
        update(most, split)
    for k in range(split, last):
        arrived(k)
    forward(last)

    @pl.when(me == 0)
    def _():
        arrive(origs.at[pl.ds(0, nb - piece)], o1_send)

    m_copy.wait_send()
    if_red(me, lambda: arrive(part.at[pl.ds(0, n_red - 1)], p1_send))
    pl.when(jnp.logical_not(is_red(me)))(lambda: arrive(part, p1_send))

    def drain():
        @pl.when(me == 0)
        def _():
            arrive(got.at[pl.ds(1, n_prow - 1)], o2_send)

        @pl.when(me > 0)
        def _():
            arrive(got.at[pl.ds(1, n_prow - 2)], o2_send)

        arrive(got.at[pl.ds(1, n_prow - 1)], p2_send)

    if_red(me, drain)

    def sent_all(lanes, sem):
        tiles = lanes * (n_y - 1) // 128
        if tiles:
            full = rows // 128
            count = next((n for n in range(1, n_pcol + 1) if tiles % n == 0 and tiles // n <= full), 0)
            parts = [(count, tiles // count)] if count else [(tiles // full, full), (1, tiles % full)]
            for count, wide in parts:
                arrive(l_full.at[pl.ds(0, count), :, pl.ds(0, wide * 128)], sem)

    shared, end = rows - bounds[tail], rows - bounds[last]
    for skip, here in ((0, me > 0), (bounds[top], me == 0)):
        @pl.when(here & (core == 0))
        def _():
            sent_all(bounds[tail] - skip, y_send)
            sent_all(bounds[tail] - skip, f_send)

        @pl.when(here & (core == 1))
        def _():
            sent_all(rows + shared + 2 * end - skip, y_send)
            sent_all(rows + shared - 2 * end - skip, f_send)


def last_update(start, in_v, l_full, u_in, out_hbm, end_v, sem):
    rows, width = in_v.shape
    nb = u_in.shape[0]
    rows_k = pl.ds(start, rows - start)
    pltpu.make_async_copy(in_v.at[pl.ds(0, start)], out_hbm.at[pl.ds(0, start)], sem).start()
    panel = l_full[:, :, rows_k].reshape(nb, rows - start)
    product = lax.dot_general(panel, u_in[...], (((0,), (0,)), ((), ())), preferred_element_type=F32)
    end_v[...] = (in_v[rows_k, :].astype(F32) - product).astype(BF16)
    pltpu.make_async_copy(end_v, out_hbm.at[rows_k], sem).start()
    pltpu.make_async_copy(in_v, out_hbm, sem).wait()


def hbm(array):
    return pltpu.with_memory_space_constraint(array, pltpu.HBM)


def chunk_bounds(rows, nb):
    last = min(5 * nb, (rows - nb) // 2)
    bounds = [0, nb]
    while bounds[-1] < rows - last:
        bounds.append(min(bounds[-1] + 4 * nb, rows - last))
    tail = len(bounds) - 1
    if last == 5 * nb:
        bounds += [rows - 2 * nb, rows - nb // 2]
    return (*bounds, rows), tail


def body(n_prow, n_pcol, a_matrix, l_panel, l_inverse, pivots):
    rows, width = a_matrix.shape
    nb = l_inverse.shape[0]
    depth = l_panel.shape[1]
    n_red = min(n_prow // 2, nb // 16)
    piece = nb // n_red
    n_y = n_pcol // CORES
    bounds, tail = chunk_bounds(rows, nb)
    chunks = len(bounds) - 1
    dma = pltpu.SemaphoreType.DMA
    flag = pltpu.SemaphoreType.REGULAR
    most_rows, l_all, u_block = pl.pallas_call(
        functools.partial(kernel, n_prow, n_pcol, bounds, tail),
        out_shape=[
            jax.ShapeDtypeStruct((rows, width), BF16),
            jax.ShapeDtypeStruct((n_pcol, depth, rows), BF16),
            jax.ShapeDtypeStruct((nb, width), BF16),
        ],
        in_specs=[pl.BlockSpec(memory_space=pl.ANY)] * 4,
        out_specs=[pl.BlockSpec(memory_space=pltpu.VMEM)] * 3,
        scratch_shapes=[
            pltpu.VMEM((rows, width), BF16),
            pltpu.VMEM((rows, nb), BF16),
            pltpu.VMEM((nb, nb), BF16),
            pltpu.VMEM((1, nb), jnp.int32),
            pltpu.VMEM((n_red, piece, width), BF16),
            pltpu.VMEM((n_prow, piece, width), BF16),
            pltpu.VMEM((piece, width), BF16),
            pltpu.VMEM((nb, width), BF16),
            pltpu.VMEM((nb, width), BF16),
            dma((2,)), dma((LOADS,)), dma((7,)), dma((5,)),
            dma((max(n_y - 1, 1), chunks)), dma((max(n_y - 1, 1), chunks)), flag((3,)),
        ],
        compiler_params=pltpu.CompilerParams(
            collective_id=0, has_side_effects=True, vmem_limit_bytes=24 * 2 ** 20),
    )(hbm(a_matrix), hbm(l_panel.T), hbm(l_inverse), hbm(pivots.reshape(1, nb)))
    start = bounds[min(tail + 1, chunks - 1)]
    return pl.pallas_call(
        functools.partial(last_update, start),
        out_shape=jax.ShapeDtypeStruct((rows, width), BF16),
        in_specs=[pl.BlockSpec(memory_space=pltpu.VMEM)] * 3,
        out_specs=pl.BlockSpec(memory_space=pltpu.HBM),
        scratch_shapes=[pltpu.VMEM((rows - start, width), BF16), dma],
        compiler_params=pltpu.CompilerParams(vmem_limit_bytes=8 * 2 ** 20),
    )(most_rows, l_all, u_block)


def solution(mesh):
    n_prow, n_pcol = mesh.shape["prow"], mesh.shape["pcol"]
    in_specs = (P("prow", "pcol"), P("prow", "pcol"), P(), P())
    return jax.shard_map(
        functools.partial(body, n_prow, n_pcol),
        mesh=mesh, in_specs=in_specs, out_specs=P("prow", "pcol"), check_vma=False)
```

```python
import functools

import jax
import jax.numpy as jnp
from jax import lax
from jax.experimental import pallas as pl
from jax.experimental.pallas import tpu as pltpu
from jax.sharding import PartitionSpec as P

MESH = pl.DeviceIdType.MESH
F32 = jnp.float32
BF16 = jnp.bfloat16
CORES = 2
LOADS = 2
ENTER_AFTER = 0


def one_hot(mask):
    return jnp.where(mask, 1.0, 0.0).astype(BF16)


def column_of(pv_row):
    nb = pv_row.shape[1]
    slot = lax.broadcasted_iota(jnp.int32, (nb, nb), 0)
    other = lax.broadcasted_iota(jnp.int32, (nb, nb), 1)
    return jnp.max(jnp.where(slot == other, pv_row, -1.0), axis=1, keepdims=True)


def swap_plan(pv_row, pv_col):
    nb = pv_row.shape[1]
    slot = lax.broadcasted_iota(jnp.int32, (nb, nb), 0).astype(F32)
    other = lax.broadcasted_iota(jnp.int32, (nb, nb), 1).astype(F32)
    slot_col = lax.broadcasted_iota(jnp.int32, (nb, 1), 0).astype(F32)
    earlier = other < slot
    pointer = jnp.max(jnp.where((pv_row == slot) & earlier, other, -1.0), axis=1, keepdims=True)
    chain = one_hot(other == jnp.where(pointer >= 0, pointer, slot_col))
    for _ in range((nb - 1).bit_length()):
        chain = jnp.dot(chain, chain, preferred_element_type=F32).astype(BF16)
    same = pv_row == pv_col
    previous = jnp.max(jnp.where(same & earlier, other, -1.0), axis=1, keepdims=True)
    via = jnp.dot(one_hot(other == previous), chain, preferred_element_type=F32).astype(BF16)
    repeated = jnp.max(jnp.where(same & (slot > other), 1.0, 0.0), axis=0, keepdims=True)
    landing = jnp.where((repeated < 0.5) & (pv_row >= nb), pv_row, -1.0)
    return previous, via, chain, landing


def kernel(
    n_prow, n_pcol, bounds, tail,
    a_hbm, l_hbm, inv_hbm, pv_hbm, out_v, l_full, u_out,
    a_v, here_v, inv_v, pv_ref, part, got, mine, tops, origs,
    load_sem, a_sem, send_sem, recv_sem, y_recv, f_recv, flags,
):
    p1_send, p2_send, o1_send, o2_send, y_send, m_send, f_send = (send_sem.at[i] for i in range(7))
    p1_recv, p2_recv, o1_recv, o2_recv, m_recv = (recv_sem.at[i] for i in range(5))
    owner_up, rest_up, mate_in = (flags.at[i] for i in range(3))
    rows, width = a_v.shape
    nb = inv_v.shape[0]
    n_red, piece, _ = part.shape
    depth = l_full.shape[1]
    n_y = n_pcol // CORES
    chunks = len(bounds) - 1
    top = sum(1 for k in range(chunks) if bounds[k + 1] <= nb)
    me = lax.axis_index("prow")
    col = lax.axis_index("pcol")
    y, core = col // CORES, col % CORES
    mate = y * CORES + (1 - core)

    def y_peer(d):
        return lax.rem(y + d, n_y) * CORES + core

    def y_from(d):
        return lax.rem(y + n_y - d, n_y) * CORES + core

    def to(d):
        return lax.rem(me + d, n_prow)

    def frm(d):
        return lax.rem(me + n_prow - d, n_prow)

    def lower(d):
        return me + d >= n_prow

    def is_red(index):
        return index < n_red

    def if_red(index, fn):
        pl.when(is_red(index))(fn)

    slot = lax.rem(me, n_red)

    barrier = pltpu.get_barrier_semaphore()
    for d in range(1, n_y):
        pl.semaphore_signal(barrier, inc=1, device_id=(me, y_peer(d)), device_id_type=MESH)

    @pl.when(core == 1)
    def _():
        pl.semaphore_signal(barrier, inc=1, device_id=(me, mate), device_id_type=MESH)

    pv_load = pltpu.make_async_copy(pv_hbm, pv_ref, load_sem.at[0])
    pv_load.start()
    block = rows // LOADS
    a_loads = [
        pltpu.make_async_copy(
            a_hbm.at[pl.ds(k * block, block)], a_v.at[pl.ds(k * block, block)], a_sem.at[k])
        for k in range(LOADS)
    ]
    for load in a_loads:
        load.start()
    for d in range(1, n_prow):
        @pl.when(is_red(me) & jnp.logical_not(lower(d)))
        def _():
            pl.semaphore_signal(barrier, inc=1, device_id=(to(d), y * CORES), device_id_type=MESH)

    l_load = pltpu.make_async_copy(l_hbm, l_full.at[col], load_sem.at[1])
    inv_load = pltpu.make_async_copy(inv_hbm, inv_v, load_sem.at[0])

    def cols(k):
        return pl.ds(bounds[k], bounds[k + 1] - bounds[k])

    def sent(k, fn):
        if bounds[k + 1] <= nb:
            pl.when(me > 0)(fn)
        else:
            fn()

    def both(chip, k):
        return l_full.at[pl.ds(chip * CORES, CORES), :, cols(k)]

    y_copies = {}
    for k in range(chunks):
        for d in range(1, n_y):
            src, dst = l_hbm.at[:, cols(k)], l_full.at[col, :, cols(k)]
            if k >= tail:
                src = dst = both(y, k)
            y_copies[d, k] = pltpu.make_async_remote_copy(
                src, dst, y_send, y_recv.at[d - 1, k], device_id=(me, y_peer(d)), device_id_type=MESH)
    last = chunks - 1
    y_twice = [
        pltpu.make_async_remote_copy(
            both(y, last), both(y, last), y_send, y_recv.at[d - 1, last],
            device_id=(me, y_peer(d) - core), device_id_type=MESH)
        for d in range(1, n_y)
    ]
    m_copy = pltpu.make_async_remote_copy(
        l_hbm, l_full.at[col], m_send, m_recv, device_id=(me, mate), device_id_type=MESH)

    def enter():
        pl.semaphore_wait(
            barrier, n_y - 1 + jnp.where(core == 0, 1 + CORES * jnp.minimum(me, n_red), 0))
        for k in range(tail):
            for d in range(1, n_y):
                sent(k, y_copies[d, k].start)
        @pl.when(core == 0)
        def _():
            pl.semaphore_signal(mate_in, inc=1, device_id=(me, mate), device_id_type=MESH)
            m_copy.start()
            for d in range(1, n_prow):
                for c in range(CORES):
                    there = (to(d), y * CORES + c)

                    @pl.when(is_red(me) & lower(d))
                    def _():
                        pl.semaphore_signal(owner_up, inc=1, device_id=there, device_id_type=MESH)

                    @pl.when(jnp.logical_not(is_red(me)) & is_red(to(d)))
                    def _():
                        pl.semaphore_signal(rest_up, inc=1, device_id=there, device_id_type=MESH)

    at_once = (core == 1) | (me == 0)
    pl.when(at_once)(enter)
    l_load.start()

    def global_rows(shape, axis, start):
        local = lax.broadcasted_iota(jnp.int32, shape, axis) + start
        return ((local // nb * n_prow + me) * nb + local % nb).astype(F32)

    pv_load.wait()
    inv_load.start()
    pv_row = pv_ref[...].astype(F32)
    pv_col = column_of(pv_row)
    total = jnp.zeros((nb, width), F32)
    for k in range(LOADS):
        a_loads[k].wait()
        pick = one_hot(pv_col == global_rows((1, block), 1, k * block))
        total = total + jnp.dot(pick, a_v[pl.ds(k * block, block), :], preferred_element_type=F32)
        if k == ENTER_AFTER:
            pl.when(jnp.logical_not(at_once))(enter)
    part[...] = total.astype(BF16).reshape(n_red, piece, width)

    @pl.when(core == 1)
    def _():
        pl.semaphore_wait(mate_in, 1)
        m_copy.start()

    p1_copies = {}
    for d in reversed(range(1, n_prow)):
        t = to(d)
        p1_copies[d] = pltpu.make_async_remote_copy(
            part.at[lax.rem(t, n_red)], got.at[d], p1_send, p1_recv,
            device_id=(t, col), device_id_type=MESH)
        pl.when(is_red(t) & lower(d))(p1_copies[d].start)

    inv_load.wait()
    pv_row = pv_ref[...].astype(F32)
    previous, via, chain, landing = swap_plan(pv_row, column_of(pv_row))

    @pl.when(me < n_red - 1)
    def _():
        pl.semaphore_wait(owner_up, n_red - 1 - me)

    o1_copies = [
        pltpu.make_async_remote_copy(
            a_v.at[pl.ds(t * piece, piece)], origs.at[pl.ds(t * piece, piece)], o1_send, o1_recv,
            device_id=(t, col), device_id_type=MESH)
        for t in range(1, n_red)
    ]
    o_local = pltpu.make_async_copy(a_v.at[pl.ds(0, nb)], origs, o1_recv)

    @pl.when(me == 0)
    def _():
        o_local.start()
        for copy in o1_copies:
            copy.start()

    for d in range(1, n_prow):
        pl.when(is_red(to(d)) & jnp.logical_not(lower(d)))(p1_copies[d].start)

    m_copy.wait_recv()
    l_load.wait()

    @pl.when(core == 1)
    def _():
        for k in range(tail, chunks):
            for d in range(1, n_y):
                if k == last:
                    y_twice[d - 1].start()
                y_copies[d, k].start()

    f_copies = {}
    for k in range(chunks):
        for d in range(1, n_y):
            src = l_full.at[y_from(d), :, cols(k)]
            if k >= tail:
                src = both(y_from(d) // CORES, k)
            f_copies[d, k] = pltpu.make_async_remote_copy(
                src, src, f_send, f_recv.at[d - 1, k], device_id=(me, mate), device_id_type=MESH)

    def forward(k):
        if k >= chunks:
            return

        def go():
            for d in range(1, n_y):
                y_copies[d, k].wait_recv()
                f_copies[d, k].start()

        if k == last:
            for d in range(1, n_y):
                y_copies[d, k].wait_recv()
        elif k >= tail:
            pl.when(core == 1)(go)
        else:
            sent(k, go)

    own_rows = origs.at[pl.ds(slot * piece, piece)]
    o2_copies, p2_copies = {}, {}
    for d in range(1, n_prow):
        o2_copies[d] = pltpu.make_async_remote_copy(
            own_rows, own_rows, o2_send, o2_recv,
            device_id=(to(d), col), device_id_type=MESH)
        p2_copies[d] = pltpu.make_async_remote_copy(
            mine, tops.at[pl.ds(slot * piece, piece)], p2_send, p2_recv,
            device_id=(to(d), col), device_id_type=MESH)

    def not_first(d, fn):
        pl.when(me + d != n_prow)(fn)

    def send_orig():
        @pl.when(me == 0)
        def _():
            o_local.wait()

        @pl.when(me > 0)
        def _():
            pltpu.make_async_remote_copy(
                a_v.at[pl.ds(0, piece)], own_rows, o1_send, o1_recv,
                device_id=(0, col), device_id_type=MESH).wait_recv()

        pl.semaphore_wait(rest_up, n_prow - n_red)
        for d in range(1, n_prow):
            not_first(d, o2_copies[d].start)

    def arrive(ref, sem):
        pltpu.make_async_copy(ref, ref, sem).wait()

    def gather(ref, sem):
        if_red(me, lambda: arrive(ref.at[pl.ds(0, nb - piece)], sem))
        pl.when(jnp.logical_not(is_red(me)))(lambda: arrive(ref, sem))

    if_red(me, send_orig)
    step = min(512, rows)
    for start in range(0, rows, step):
        rows_k = pl.ds(start, step)
        here = one_hot(landing == global_rows((step, 1), 0, start))
        here_v[rows_k, :] = here
        hit = jnp.dot(here, jnp.ones((nb, width), BF16), preferred_element_type=F32)
        out_v[rows_k, :] = jnp.where(hit > 0.5, 0.0, a_v[rows_k, :].astype(F32)).astype(BF16)

    forward(0)

    def reduce_and_send():
        acc = part[slot].astype(F32)
        arrive(got.at[pl.ds(1, n_prow - 1)], p1_recv)
        for d in range(1, n_prow):
            acc = acc + got[d].astype(F32)
        mine[...] = acc.astype(BF16)
        tops[pl.ds(slot * piece, piece), :] = acc.astype(BF16)
        for d in range(1, n_prow):
            pl.when(me + d == n_prow)(p2_copies[d].start)
        for d in range(1, n_prow):
            not_first(d, p2_copies[d].start)

    if_red(me, reduce_and_send)
    forward(1)
    forward(2)

    late = [tail - 1] if tail - 1 > 2 else []
    far = (core == 1) | (me >= n_prow * 3 // 4)
    for k in late:
        pl.when(far)(functools.partial(forward, k))

    pl.when(me > 0)(lambda: gather(origs, o2_recv))
    orig = origs[...]
    moved = jnp.dot(chain, orig, preferred_element_type=F32).astype(BF16)
    again = jnp.dot(via, orig, preferred_element_type=F32).astype(BF16)
    for start in range(0, rows, step):
        rows_k = pl.ds(start, step)
        landed = jnp.dot(here_v[rows_k, :], moved, preferred_element_type=F32)
        out_v[rows_k, :] = (out_v[rows_k, :].astype(F32) + landed).astype(BF16)

    for k in late:
        pl.when(jnp.logical_not(far))(functools.partial(forward, k))
    if tail < last:
        forward(tail)
    gather(tops, p2_recv)
    top_rows = jnp.where(previous >= 0, again, tops[...])
    u_block = jnp.dot(inv_v[...], top_rows, preferred_element_type=F32).astype(BF16)

    def arrived(k):
        def go():
            for d in range(1, n_y):
                f_copies[d, k].wait_recv()
        if last > k >= tail:
            pl.when(core == 0)(go)
        elif k < tail:
            sent(k, go)

    def update(first, last):
        for k in range(first, last):
            arrived(k)
        start, stop = bounds[first], bounds[last]
        rows_k = pl.ds(start, stop - start)
        panel = l_full[:, :, rows_k].reshape(nb, stop - start)
        product = lax.dot_general(
            panel, u_block, (((0,), (0,)), ((), ())), preferred_element_type=F32)
        out_v[rows_k, :] = (out_v[rows_k, :].astype(F32) - product).astype(BF16)

    most = max(top, tail - 1)

    @pl.when(me > 0)
    def _():
        update(0, most)

    @pl.when(me == 0)
    def _():
        out_v[pl.ds(0, bounds[top]), :] = u_block[:bounds[top], :]
        if most > top:
            update(top, most)

    u_out[...] = u_block
    for k in range(tail + 1, last):
        forward(k)
    split = min(tail + 1, last)
    if split > most:
        update(most, split)
    for k in range(split, last):
        arrived(k)
    forward(last)

    @pl.when(me == 0)
    def _():
        arrive(origs.at[pl.ds(0, nb - piece)], o1_send)

    m_copy.wait_send()
    if_red(me, lambda: arrive(part.at[pl.ds(0, n_red - 1)], p1_send))
    pl.when(jnp.logical_not(is_red(me)))(lambda: arrive(part, p1_send))

    def drain():
        @pl.when(me == 0)
        def _():
            arrive(got.at[pl.ds(1, n_prow - 1)], o2_send)

        @pl.when(me > 0)
        def _():
            arrive(got.at[pl.ds(1, n_prow - 2)], o2_send)

        arrive(got.at[pl.ds(1, n_prow - 1)], p2_send)

    if_red(me, drain)

    def sent_all(lanes, sem):
        tiles = lanes * (n_y - 1) // 128
        if tiles:
            full = rows // 128
            count = next((n for n in range(1, n_pcol + 1) if tiles % n == 0 and tiles // n <= full), 0)
            parts = [(count, tiles // count)] if count else [(tiles // full, full), (1, tiles % full)]
            for count, wide in parts:
                arrive(l_full.at[pl.ds(0, count), :, pl.ds(0, wide * 128)], sem)

    shared, end = rows - bounds[tail], rows - bounds[last]
    for skip, here in ((0, me > 0), (bounds[top], me == 0)):
        @pl.when(here & (core == 0))
        def _():
            sent_all(bounds[tail] - skip, y_send)
            sent_all(bounds[tail] - skip, f_send)

        @pl.when(here & (core == 1))
        def _():
            sent_all(rows + shared + 2 * end - skip, y_send)
            sent_all(rows + shared - 2 * end - skip, f_send)


def last_update(start, in_v, l_full, u_in, out_hbm, end_v, sem):
    rows, width = in_v.shape
    nb = u_in.shape[0]
    rows_k = pl.ds(start, rows - start)
    pltpu.make_async_copy(in_v.at[pl.ds(0, start)], out_hbm.at[pl.ds(0, start)], sem).start()
    panel = l_full[:, :, rows_k].reshape(nb, rows - start)
    product = lax.dot_general(panel, u_in[...], (((0,), (0,)), ((), ())), preferred_element_type=F32)
    end_v[...] = (in_v[rows_k, :].astype(F32) - product).astype(BF16)
    pltpu.make_async_copy(end_v, out_hbm.at[rows_k], sem).start()
    pltpu.make_async_copy(in_v, out_hbm, sem).wait()


def hbm(array):
    return pltpu.with_memory_space_constraint(array, pltpu.HBM)


def chunk_bounds(rows, nb):
    last = min(5 * nb, (rows - nb) // 2)
    bounds = [0, nb]
    while bounds[-1] < rows - last:
        bounds.append(min(bounds[-1] + 4 * nb, rows - last))
    tail = len(bounds) - 1
    if last == 5 * nb:
        bounds += [rows - 2 * nb, rows - nb // 2]
    return (*bounds, rows), tail


def body(n_prow, n_pcol, a_matrix, l_panel, l_inverse, pivots):
    rows, width = a_matrix.shape
    nb = l_inverse.shape[0]
    depth = l_panel.shape[1]
    n_red = min(n_prow // 2, nb // 16)
    piece = nb // n_red
    n_y = n_pcol // CORES
    bounds, tail = chunk_bounds(rows, nb)
    chunks = len(bounds) - 1
    dma = pltpu.SemaphoreType.DMA
    flag = pltpu.SemaphoreType.REGULAR
    most_rows, l_all, u_block = pl.pallas_call(
        functools.partial(kernel, n_prow, n_pcol, bounds, tail),
        out_shape=[
            jax.ShapeDtypeStruct((rows, width), BF16),
            jax.ShapeDtypeStruct((n_pcol, depth, rows), BF16),
            jax.ShapeDtypeStruct((nb, width), BF16),
        ],
        in_specs=[pl.BlockSpec(memory_space=pl.ANY)] * 4,
        out_specs=[pl.BlockSpec(memory_space=pltpu.VMEM)] * 3,
        scratch_shapes=[
            pltpu.VMEM((rows, width), BF16),
            pltpu.VMEM((rows, nb), BF16),
            pltpu.VMEM((nb, nb), BF16),
            pltpu.VMEM((1, nb), jnp.int32),
            pltpu.VMEM((n_red, piece, width), BF16),
            pltpu.VMEM((n_prow, piece, width), BF16),
            pltpu.VMEM((piece, width), BF16),
            pltpu.VMEM((nb, width), BF16),
            pltpu.VMEM((nb, width), BF16),
            dma((2,)), dma((LOADS,)), dma((7,)), dma((5,)),
            dma((max(n_y - 1, 1), chunks)), dma((max(n_y - 1, 1), chunks)), flag((3,)),
        ],
        compiler_params=pltpu.CompilerParams(
            collective_id=0, has_side_effects=True, vmem_limit_bytes=24 * 2 ** 20),
    )(hbm(a_matrix), hbm(l_panel.T), hbm(l_inverse), hbm(pivots.reshape(1, nb)))
    start = bounds[min(tail + 1, chunks - 1)]
    return pl.pallas_call(
        functools.partial(last_update, start),
        out_shape=jax.ShapeDtypeStruct((rows, width), BF16),
        in_specs=[pl.BlockSpec(memory_space=pltpu.VMEM)] * 3,
        out_specs=pl.BlockSpec(memory_space=pltpu.HBM),
        scratch_shapes=[pltpu.VMEM((rows - start, width), BF16), dma],
        compiler_params=pltpu.CompilerParams(vmem_limit_bytes=8 * 2 ** 20),
    )(most_rows, l_all, u_block)


def solution(mesh):
    n_prow, n_pcol = mesh.shape["prow"], mesh.shape["pcol"]
    in_specs = (P("prow", "pcol"), P("prow", "pcol"), P(), P())
    return jax.shard_map(
        functools.partial(body, n_prow, n_pcol),
        mesh=mesh, in_specs=in_specs, out_specs=P("prow", "pcol"), check_vma=False)
```

```python
import functools

import jax
import jax.numpy as jnp
from jax import lax
from jax.experimental import pallas as pl
from jax.experimental.pallas import tpu as pltpu
from jax.sharding import PartitionSpec as P

MESH = pl.DeviceIdType.MESH
F32 = jnp.float32
BF16 = jnp.bfloat16
CORES = 2
LOADS = 2
ENTER_AFTER = 0


def one_hot(mask):
    return jnp.where(mask, 1.0, 0.0).astype(BF16)


def column_of(pv_row):
    nb = pv_row.shape[1]
    slot = lax.broadcasted_iota(jnp.int32, (nb, nb), 0)
    other = lax.broadcasted_iota(jnp.int32, (nb, nb), 1)
    return jnp.max(jnp.where(slot == other, pv_row, -1.0), axis=1, keepdims=True)


def swap_plan(pv_row, pv_col):
    nb = pv_row.shape[1]
    slot = lax.broadcasted_iota(jnp.int32, (nb, nb), 0).astype(F32)
    other = lax.broadcasted_iota(jnp.int32, (nb, nb), 1).astype(F32)
    slot_col = lax.broadcasted_iota(jnp.int32, (nb, 1), 0).astype(F32)
    earlier = other < slot
    pointer = jnp.max(jnp.where((pv_row == slot) & earlier, other, -1.0), axis=1, keepdims=True)
    chain = one_hot(other == jnp.where(pointer >= 0, pointer, slot_col))
    for _ in range((nb - 1).bit_length()):
        chain = jnp.dot(chain, chain, preferred_element_type=F32).astype(BF16)
    same = pv_row == pv_col
    previous = jnp.max(jnp.where(same & earlier, other, -1.0), axis=1, keepdims=True)
    via = jnp.dot(one_hot(other == previous), chain, preferred_element_type=F32).astype(BF16)
    repeated = jnp.max(jnp.where(same & (slot > other), 1.0, 0.0), axis=0, keepdims=True)
    landing = jnp.where((repeated < 0.5) & (pv_row >= nb), pv_row, -1.0)
    return previous, via, chain, landing


def kernel(
    n_prow, n_pcol, bounds, tail,
    a_hbm, l_hbm, inv_hbm, pv_hbm, out_v, l_full, u_out,
    a_v, here_v, inv_v, pv_ref, part, got, mine, tops, origs,
    load_sem, a_sem, send_sem, recv_sem, y_recv, f_recv, flags,
):
    p1_send, p2_send, o1_send, o2_send, y_send, m_send, f_send = (send_sem.at[i] for i in range(7))
    p1_recv, p2_recv, o1_recv, o2_recv, m_recv = (recv_sem.at[i] for i in range(5))
    owner_up, rest_up, mate_in = (flags.at[i] for i in range(3))
    rows, width = a_v.shape
    nb = inv_v.shape[0]
    n_red, piece, _ = part.shape
    depth = l_full.shape[1]
    n_y = n_pcol // CORES
    chunks = len(bounds) - 1
    top = sum(1 for k in range(chunks) if bounds[k + 1] <= nb)
    me = lax.axis_index("prow")
    col = lax.axis_index("pcol")
    y, core = col // CORES, col % CORES
    mate = y * CORES + (1 - core)

    def y_peer(d):
        return lax.rem(y + d, n_y) * CORES + core

    def y_from(d):
        return lax.rem(y + n_y - d, n_y) * CORES + core

    def to(d):
        return lax.rem(me + d, n_prow)

    def frm(d):
        return lax.rem(me + n_prow - d, n_prow)

    def lower(d):
        return me + d >= n_prow

    def is_red(index):
        return index < n_red

    def if_red(index, fn):
        pl.when(is_red(index))(fn)

    slot = lax.rem(me, n_red)

    barrier = pltpu.get_barrier_semaphore()
    for d in range(1, n_y):
        pl.semaphore_signal(barrier, inc=1, device_id=(me, y_peer(d)), device_id_type=MESH)

    @pl.when(core == 1)
    def _():
        pl.semaphore_signal(barrier, inc=1, device_id=(me, mate), device_id_type=MESH)

    pv_load = pltpu.make_async_copy(pv_hbm, pv_ref, load_sem.at[0])
    pv_load.start()
    block = rows // LOADS
    a_loads = [
        pltpu.make_async_copy(
            a_hbm.at[pl.ds(k * block, block)], a_v.at[pl.ds(k * block, block)], a_sem.at[k])
        for k in range(LOADS)
    ]
    for load in a_loads:
        load.start()
    for d in range(1, n_prow):
        @pl.when(is_red(me) & jnp.logical_not(lower(d)))
        def _():
            pl.semaphore_signal(barrier, inc=1, device_id=(to(d), y * CORES), device_id_type=MESH)

    l_load = pltpu.make_async_copy(l_hbm, l_full.at[col], load_sem.at[1])
    inv_load = pltpu.make_async_copy(inv_hbm, inv_v, load_sem.at[0])

    def cols(k):
        return pl.ds(bounds[k], bounds[k + 1] - bounds[k])

    def sent(k, fn):
        if bounds[k + 1] <= nb:
            pl.when(me > 0)(fn)
        else:
            fn()

    def both(chip, k):
        return l_full.at[pl.ds(chip * CORES, CORES), :, cols(k)]

    y_copies = {}
    for k in range(chunks):
        for d in range(1, n_y):
            src, dst = l_hbm.at[:, cols(k)], l_full.at[col, :, cols(k)]
            if k >= tail:
                src = dst = both(y, k)
            y_copies[d, k] = pltpu.make_async_remote_copy(
                src, dst, y_send, y_recv.at[d - 1, k], device_id=(me, y_peer(d)), device_id_type=MESH)
    last = chunks - 1
    y_twice = [
        pltpu.make_async_remote_copy(
            both(y, last), both(y, last), y_send, y_recv.at[d - 1, last],
            device_id=(me, y_peer(d) - core), device_id_type=MESH)
        for d in range(1, n_y)
    ]
    m_copy = pltpu.make_async_remote_copy(
        l_hbm, l_full.at[col], m_send, m_recv, device_id=(me, mate), device_id_type=MESH)

    def enter():
        pl.semaphore_wait(
            barrier, n_y - 1 + jnp.where(core == 0, 1 + CORES * jnp.minimum(me, n_red), 0))
        for k in range(tail):
            for d in range(1, n_y):
                sent(k, y_copies[d, k].start)
        @pl.when(core == 0)
        def _():
            pl.semaphore_signal(mate_in, inc=1, device_id=(me, mate), device_id_type=MESH)
            m_copy.start()
            for d in range(1, n_prow):
                for c in range(CORES):
                    there = (to(d), y * CORES + c)

                    @pl.when(is_red(me) & lower(d))
                    def _():
                        pl.semaphore_signal(owner_up, inc=1, device_id=there, device_id_type=MESH)

                    @pl.when(jnp.logical_not(is_red(me)) & is_red(to(d)))
                    def _():
                        pl.semaphore_signal(rest_up, inc=1, device_id=there, device_id_type=MESH)

    at_once = (core == 1) | (me == 0)
    pl.when(at_once)(enter)
    l_load.start()

    def global_rows(shape, axis, start):
        local = lax.broadcasted_iota(jnp.int32, shape, axis) + start
        return ((local // nb * n_prow + me) * nb + local % nb).astype(F32)

    pv_load.wait()
    inv_load.start()
    pv_row = pv_ref[...].astype(F32)
    pv_col = column_of(pv_row)
    total = jnp.zeros((nb, width), F32)
    for k in range(LOADS):
        a_loads[k].wait()
        pick = one_hot(pv_col == global_rows((1, block), 1, k * block))
        total = total + jnp.dot(pick, a_v[pl.ds(k * block, block), :], preferred_element_type=F32)
        if k == ENTER_AFTER:
            pl.when(jnp.logical_not(at_once))(enter)
    part[...] = total.astype(BF16).reshape(n_red, piece, width)

    @pl.when(core == 1)
    def _():
        pl.semaphore_wait(mate_in, 1)
        m_copy.start()

    p1_copies = {}
    for d in reversed(range(1, n_prow)):
        t = to(d)
        p1_copies[d] = pltpu.make_async_remote_copy(
            part.at[lax.rem(t, n_red)], got.at[d], p1_send, p1_recv,
            device_id=(t, col), device_id_type=MESH)
        pl.when(is_red(t) & lower(d))(p1_copies[d].start)

    inv_load.wait()
    pv_row = pv_ref[...].astype(F32)
    previous, via, chain, landing = swap_plan(pv_row, column_of(pv_row))

    @pl.when(me < n_red - 1)
    def _():
        pl.semaphore_wait(owner_up, n_red - 1 - me)

    o1_copies = [
        pltpu.make_async_remote_copy(
            a_v.at[pl.ds(t * piece, piece)], origs.at[pl.ds(t * piece, piece)], o1_send, o1_recv,
            device_id=(t, col), device_id_type=MESH)
        for t in range(1, n_red)
    ]
    o_local = pltpu.make_async_copy(a_v.at[pl.ds(0, nb)], origs, o1_recv)

    @pl.when(me == 0)
    def _():
        o_local.start()
        for copy in o1_copies:
            copy.start()

    for d in range(1, n_prow):
        pl.when(is_red(to(d)) & jnp.logical_not(lower(d)))(p1_copies[d].start)

    m_copy.wait_recv()
    l_load.wait()

    @pl.when(core == 1)
    def _():
        for k in range(tail, chunks):
            for d in range(1, n_y):
                if k == last:
                    y_twice[d - 1].start()
                y_copies[d, k].start()

    f_copies = {}
    for k in range(chunks):
        for d in range(1, n_y):
            src = l_full.at[y_from(d), :, cols(k)]
            if k >= tail:
                src = both(y_from(d) // CORES, k)
            f_copies[d, k] = pltpu.make_async_remote_copy(
                src, src, f_send, f_recv.at[d - 1, k], device_id=(me, mate), device_id_type=MESH)

    def forward(k):
        if k >= chunks:
            return

        def go():
            for d in range(1, n_y):
                y_copies[d, k].wait_recv()
                f_copies[d, k].start()

        if k == last:
            for d in range(1, n_y):
                y_copies[d, k].wait_recv()
        elif k >= tail:
            pl.when(core == 1)(go)
        else:
            sent(k, go)

    own_rows = origs.at[pl.ds(slot * piece, piece)]
    o2_copies, p2_copies = {}, {}
    for d in range(1, n_prow):
        o2_copies[d] = pltpu.make_async_remote_copy(
            own_rows, own_rows, o2_send, o2_recv,
            device_id=(to(d), col), device_id_type=MESH)
        p2_copies[d] = pltpu.make_async_remote_copy(
            mine, tops.at[pl.ds(slot * piece, piece)], p2_send, p2_recv,
            device_id=(to(d), col), device_id_type=MESH)

    def not_first(d, fn):
        pl.when(me + d != n_prow)(fn)

    def send_orig():
        @pl.when(me == 0)
        def _():
            o_local.wait()

        @pl.when(me > 0)
        def _():
            pltpu.make_async_remote_copy(
                a_v.at[pl.ds(0, piece)], own_rows, o1_send, o1_recv,
                device_id=(0, col), device_id_type=MESH).wait_recv()

        pl.semaphore_wait(rest_up, n_prow - n_red)
        for d in range(1, n_prow):
            not_first(d, o2_copies[d].start)

    def arrive(ref, sem):
        pltpu.make_async_copy(ref, ref, sem).wait()

    def gather(ref, sem):
        if_red(me, lambda: arrive(ref.at[pl.ds(0, nb - piece)], sem))
        pl.when(jnp.logical_not(is_red(me)))(lambda: arrive(ref, sem))

    if_red(me, send_orig)
    def reduce_and_send():
        acc = part[slot].astype(F32)
        arrive(got.at[pl.ds(1, n_prow - 1)], p1_recv)
        for d in range(1, n_prow):
            acc = acc + got[d].astype(F32)
        mine[...] = acc.astype(BF16)
        tops[pl.ds(slot * piece, piece), :] = acc.astype(BF16)
        for d in range(1, n_prow):
            pl.when(me + d == n_prow)(p2_copies[d].start)
        for d in range(1, n_prow):
            not_first(d, p2_copies[d].start)

    pl.when((me > 0) & is_red(me))(reduce_and_send)

    step = min(512, rows)
    for start in range(0, rows, step):
        rows_k = pl.ds(start, step)
        here = one_hot(landing == global_rows((step, 1), 0, start))
        here_v[rows_k, :] = here
        hit = jnp.dot(here, jnp.ones((nb, width), BF16), preferred_element_type=F32)
        out_v[rows_k, :] = jnp.where(hit > 0.5, 0.0, a_v[rows_k, :].astype(F32)).astype(BF16)

    forward(0)

    pl.when(me == 0)(reduce_and_send)
    forward(1)
    forward(2)

    late = [tail - 1] if tail - 1 > 2 else []
    far = (core == 1) | (me >= n_prow * 3 // 4)
    for k in late:
        pl.when(far)(functools.partial(forward, k))

    pl.when(me > 0)(lambda: gather(origs, o2_recv))
    orig = origs[...]
    moved = jnp.dot(chain, orig, preferred_element_type=F32).astype(BF16)
    again = jnp.dot(via, orig, preferred_element_type=F32).astype(BF16)
    for start in range(0, rows, step):
        rows_k = pl.ds(start, step)
        landed = jnp.dot(here_v[rows_k, :], moved, preferred_element_type=F32)
        out_v[rows_k, :] = (out_v[rows_k, :].astype(F32) + landed).astype(BF16)

    for k in late:
        pl.when(jnp.logical_not(far))(functools.partial(forward, k))
    if tail < last:
        forward(tail)
    gather(tops, p2_recv)
    top_rows = jnp.where(previous >= 0, again, tops[...])
    u_block = jnp.dot(inv_v[...], top_rows, preferred_element_type=F32).astype(BF16)

    def arrived(k):
        def go():
            for d in range(1, n_y):
                f_copies[d, k].wait_recv()
        if last > k >= tail:
            pl.when(core == 0)(go)
        elif k < tail:
            sent(k, go)

    def update(first, last):
        for k in range(first, last):
            arrived(k)
        start, stop = bounds[first], bounds[last]
        rows_k = pl.ds(start, stop - start)
        panel = l_full[:, :, rows_k].reshape(nb, stop - start)
        product = lax.dot_general(
            panel, u_block, (((0,), (0,)), ((), ())), preferred_element_type=F32)
        out_v[rows_k, :] = (out_v[rows_k, :].astype(F32) - product).astype(BF16)

    most = max(top, tail - 1)

    @pl.when(me > 0)
    def _():
        update(0, most)

    @pl.when(me == 0)
    def _():
        out_v[pl.ds(0, bounds[top]), :] = u_block[:bounds[top], :]
        if most > top:
            update(top, most)

    u_out[...] = u_block
    for k in range(tail + 1, last):
        forward(k)
    split = min(tail + 1, last)
    if split > most:
        update(most, split)
    for k in range(split, last):
        arrived(k)
    forward(last)

    @pl.when(me == 0)
    def _():
        arrive(origs.at[pl.ds(0, nb - piece)], o1_send)

    m_copy.wait_send()
    if_red(me, lambda: arrive(part.at[pl.ds(0, n_red - 1)], p1_send))
    pl.when(jnp.logical_not(is_red(me)))(lambda: arrive(part, p1_send))

    def drain():
        @pl.when(me == 0)
        def _():
            arrive(got.at[pl.ds(1, n_prow - 1)], o2_send)

        @pl.when(me > 0)
        def _():
            arrive(got.at[pl.ds(1, n_prow - 2)], o2_send)

        arrive(got.at[pl.ds(1, n_prow - 1)], p2_send)

    if_red(me, drain)

    def sent_all(lanes, sem):
        tiles = lanes * (n_y - 1) // 128
        if tiles:
            full = rows // 128
            count = next((n for n in range(1, n_pcol + 1) if tiles % n == 0 and tiles // n <= full), 0)
            parts = [(count, tiles // count)] if count else [(tiles // full, full), (1, tiles % full)]
            for count, wide in parts:
                arrive(l_full.at[pl.ds(0, count), :, pl.ds(0, wide * 128)], sem)

    shared, end = rows - bounds[tail], rows - bounds[last]
    for skip, here in ((0, me > 0), (bounds[top], me == 0)):
        @pl.when(here & (core == 0))
        def _():
            sent_all(bounds[tail] - skip, y_send)
            sent_all(bounds[tail] - skip, f_send)

        @pl.when(here & (core == 1))
        def _():
            sent_all(rows + shared + 2 * end - skip, y_send)
            sent_all(rows + shared - 2 * end - skip, f_send)


def last_update(start, in_v, l_full, u_in, out_hbm, end_v, sem):
    rows, width = in_v.shape
    nb = u_in.shape[0]
    rows_k = pl.ds(start, rows - start)
    pltpu.make_async_copy(in_v.at[pl.ds(0, start)], out_hbm.at[pl.ds(0, start)], sem).start()
    panel = l_full[:, :, rows_k].reshape(nb, rows - start)
    product = lax.dot_general(panel, u_in[...], (((0,), (0,)), ((), ())), preferred_element_type=F32)
    end_v[...] = (in_v[rows_k, :].astype(F32) - product).astype(BF16)
    pltpu.make_async_copy(end_v, out_hbm.at[rows_k], sem).start()
    pltpu.make_async_copy(in_v, out_hbm, sem).wait()


def hbm(array):
    return pltpu.with_memory_space_constraint(array, pltpu.HBM)


def chunk_bounds(rows, nb):
    last = min(5 * nb, (rows - nb) // 2)
    bounds = [0, nb]
    while bounds[-1] < rows - last:
        bounds.append(min(bounds[-1] + 4 * nb, rows - last))
    tail = len(bounds) - 1
    if last == 5 * nb:
        bounds += [rows - 2 * nb, rows - nb // 2]
    return (*bounds, rows), tail


def body(n_prow, n_pcol, a_matrix, l_panel, l_inverse, pivots):
    rows, width = a_matrix.shape
    nb = l_inverse.shape[0]
    depth = l_panel.shape[1]
    n_red = min(n_prow // 2, nb // 16)
    piece = nb // n_red
    n_y = n_pcol // CORES
    bounds, tail = chunk_bounds(rows, nb)
    chunks = len(bounds) - 1
    dma = pltpu.SemaphoreType.DMA
    flag = pltpu.SemaphoreType.REGULAR
    most_rows, l_all, u_block = pl.pallas_call(
        functools.partial(kernel, n_prow, n_pcol, bounds, tail),
        out_shape=[
            jax.ShapeDtypeStruct((rows, width), BF16),
            jax.ShapeDtypeStruct((n_pcol, depth, rows), BF16),
            jax.ShapeDtypeStruct((nb, width), BF16),
        ],
        in_specs=[pl.BlockSpec(memory_space=pl.ANY)] * 4,
        out_specs=[pl.BlockSpec(memory_space=pltpu.VMEM)] * 3,
        scratch_shapes=[
            pltpu.VMEM((rows, width), BF16),
            pltpu.VMEM((rows, nb), BF16),
            pltpu.VMEM((nb, nb), BF16),
            pltpu.VMEM((1, nb), jnp.int32),
            pltpu.VMEM((n_red, piece, width), BF16),
            pltpu.VMEM((n_prow, piece, width), BF16),
            pltpu.VMEM((piece, width), BF16),
            pltpu.VMEM((nb, width), BF16),
            pltpu.VMEM((nb, width), BF16),
            dma((2,)), dma((LOADS,)), dma((7,)), dma((5,)),
            dma((max(n_y - 1, 1), chunks)), dma((max(n_y - 1, 1), chunks)), flag((3,)),
        ],
        compiler_params=pltpu.CompilerParams(
            collective_id=0, has_side_effects=True, vmem_limit_bytes=24 * 2 ** 20),
    )(hbm(a_matrix), hbm(l_panel.T), hbm(l_inverse), hbm(pivots.reshape(1, nb)))
    start = bounds[min(tail + 1, chunks - 1)]
    return pl.pallas_call(
        functools.partial(last_update, start),
        out_shape=jax.ShapeDtypeStruct((rows, width), BF16),
        in_specs=[pl.BlockSpec(memory_space=pltpu.VMEM)] * 3,
        out_specs=pl.BlockSpec(memory_space=pltpu.HBM),
        scratch_shapes=[pltpu.VMEM((rows - start, width), BF16), dma],
        compiler_params=pltpu.CompilerParams(vmem_limit_bytes=8 * 2 ** 20),
    )(most_rows, l_all, u_block)


def solution(mesh):
    n_prow, n_pcol = mesh.shape["prow"], mesh.shape["pcol"]
    in_specs = (P("prow", "pcol"), P("prow", "pcol"), P(), P())
    return jax.shard_map(
        functools.partial(body, n_prow, n_pcol),
        mesh=mesh, in_specs=in_specs, out_specs=P("prow", "pcol"), check_vma=False)
```

```python
import functools

import jax
import jax.numpy as jnp
from jax import lax
from jax.experimental import pallas as pl
from jax.experimental.pallas import tpu as pltpu
from jax.sharding import PartitionSpec as P

MESH = pl.DeviceIdType.MESH
F32 = jnp.float32
BF16 = jnp.bfloat16
CORES = 2
LOADS = 2
ENTER_AFTER = 0


def one_hot(mask):
    return jnp.where(mask, 1.0, 0.0).astype(BF16)


def column_of(pv_row):
    nb = pv_row.shape[1]
    slot = lax.broadcasted_iota(jnp.int32, (nb, nb), 0)
    other = lax.broadcasted_iota(jnp.int32, (nb, nb), 1)
    return jnp.max(jnp.where(slot == other, pv_row, -1.0), axis=1, keepdims=True)


def swap_plan(pv_row, pv_col):
    nb = pv_row.shape[1]
    slot = lax.broadcasted_iota(jnp.int32, (nb, nb), 0).astype(F32)
    other = lax.broadcasted_iota(jnp.int32, (nb, nb), 1).astype(F32)
    slot_col = lax.broadcasted_iota(jnp.int32, (nb, 1), 0).astype(F32)
    earlier = other < slot
    pointer = jnp.max(jnp.where((pv_row == slot) & earlier, other, -1.0), axis=1, keepdims=True)
    chain = one_hot(other == jnp.where(pointer >= 0, pointer, slot_col))
    for _ in range((nb - 1).bit_length()):
        chain = jnp.dot(chain, chain, preferred_element_type=F32).astype(BF16)
    same = pv_row == pv_col
    previous = jnp.max(jnp.where(same & earlier, other, -1.0), axis=1, keepdims=True)
    via = jnp.dot(one_hot(other == previous), chain, preferred_element_type=F32).astype(BF16)
    repeated = jnp.max(jnp.where(same & (slot > other), 1.0, 0.0), axis=0, keepdims=True)
    landing = jnp.where((repeated < 0.5) & (pv_row >= nb), pv_row, -1.0)
    return previous, via, chain, landing


def kernel(
    n_prow, n_pcol, bounds, tail,
    a_hbm, l_hbm, inv_hbm, pv_hbm, out_v, l_full, u_out,
    a_v, here_v, inv_v, pv_ref, part, got, mine, tops, origs,
    load_sem, a_sem, send_sem, recv_sem, y_recv, f_recv, flags,
):
    p1_send = p2_send = o1_send = o2_send = send_sem.at[0]
    y_send = m_send = f_send = send_sem.at[1]
    p1_recv, p2_recv, o1_recv, o2_recv, m_recv = (recv_sem.at[i] for i in range(5))
    owner_up, rest_up, mate_in = (flags.at[i] for i in range(3))
    rows, width = a_v.shape
    nb = inv_v.shape[0]
    n_red, piece, _ = part.shape
    depth = l_full.shape[1]
    n_y = n_pcol // CORES
    chunks = len(bounds) - 1
    me = lax.axis_index("prow")
    col = lax.axis_index("pcol")
    y, core = col // CORES, col % CORES
    mate = y * CORES + (1 - core)

    def y_peer(d):
        return lax.rem(y + d, n_y) * CORES + core

    def y_from(d):
        return lax.rem(y + n_y - d, n_y) * CORES + core

    def to(d):
        return lax.rem(me + d, n_prow)

    def frm(d):
        return lax.rem(me + n_prow - d, n_prow)

    def lower(d):
        return me + d >= n_prow

    def is_red(index):
        return index < n_red

    def if_red(index, fn):
        pl.when(is_red(index))(fn)

    slot = lax.rem(me, n_red)

    barrier = pltpu.get_barrier_semaphore()
    for d in range(1, n_y):
        pl.semaphore_signal(barrier, inc=1, device_id=(me, y_peer(d)), device_id_type=MESH)

    @pl.when(core == 1)
    def _():
        pl.semaphore_signal(barrier, inc=1, device_id=(me, mate), device_id_type=MESH)

    pv_load = pltpu.make_async_copy(pv_hbm, pv_ref, load_sem.at[0])
    pv_load.start()
    block = rows // LOADS
    a_loads = [
        pltpu.make_async_copy(
            a_hbm.at[pl.ds(k * block, block)], a_v.at[pl.ds(k * block, block)], a_sem.at[k])
        for k in range(LOADS)
    ]
    for load in a_loads:
        load.start()
    for d in range(1, n_prow):
        @pl.when(is_red(me) & jnp.logical_not(lower(d)))
        def _():
            pl.semaphore_signal(barrier, inc=1, device_id=(to(d), y * CORES), device_id_type=MESH)

    l_load = pltpu.make_async_copy(l_hbm, l_full.at[col], load_sem.at[1])
    inv_load = pltpu.make_async_copy(inv_hbm, inv_v, load_sem.at[0])

    def cols(k):
        return pl.ds(bounds[k], bounds[k + 1] - bounds[k])

    def sent(k, fn):
        if k == 0:
            pl.when(me > 0)(lambda: fn(cols(k)))
            pl.when(me == 0)(lambda: fn(pl.ds(nb, bounds[1] - nb)))
        else:
            fn(cols(k))

    def both(chip, k):
        return l_full.at[pl.ds(chip * CORES, CORES), :, cols(k)]

    def y_copy(d, k, at):
        src, dst = l_hbm.at[:, at], l_full.at[col, :, at]
        if k >= tail:
            src = dst = both(y, k)
        return pltpu.make_async_remote_copy(
            src, dst, y_send, y_recv.at[d - 1, k], device_id=(me, y_peer(d)), device_id_type=MESH)

    last = chunks - 1
    y_twice = [
        pltpu.make_async_remote_copy(
            both(y, last), both(y, last), y_send, y_recv.at[d - 1, last],
            device_id=(me, y_peer(d) - core), device_id_type=MESH)
        for d in range(1, n_y)
    ]
    m_copy = pltpu.make_async_remote_copy(
        l_hbm, l_full.at[col], m_send, m_recv, device_id=(me, mate), device_id_type=MESH)

    def enter():
        pl.semaphore_wait(
            barrier, n_y - 1 + jnp.where(core == 0, 1 + CORES * jnp.minimum(me, n_red), 0))
        for k in range(tail):
            for d in range(1, n_y):
                sent(k, lambda at: y_copy(d, k, at).start())
        @pl.when(core == 0)
        def _():
            pl.semaphore_signal(mate_in, inc=1, device_id=(me, mate), device_id_type=MESH)
            m_copy.start()
            for d in range(1, n_prow):
                for c in range(CORES):
                    there = (to(d), y * CORES + c)

                    @pl.when(is_red(me) & lower(d))
                    def _():
                        pl.semaphore_signal(owner_up, inc=1, device_id=there, device_id_type=MESH)

                    @pl.when(jnp.logical_not(is_red(me)) & is_red(to(d)))
                    def _():
                        pl.semaphore_signal(rest_up, inc=1, device_id=there, device_id_type=MESH)

    at_once = (core == 1) | (me == 0)
    pl.when(at_once)(enter)
    l_load.start()

    def global_rows(shape, axis, start):
        local = lax.broadcasted_iota(jnp.int32, shape, axis) + start
        return ((local // nb * n_prow + me) * nb + local % nb).astype(F32)

    pv_load.wait()
    inv_load.start()
    pv_row = pv_ref[...].astype(F32)
    pv_col = column_of(pv_row)
    total = jnp.zeros((nb, width), F32)
    for k in range(LOADS):
        a_loads[k].wait()
        pick = one_hot(pv_col == global_rows((1, block), 1, k * block))
        total = total + jnp.dot(pick, a_v[pl.ds(k * block, block), :], preferred_element_type=F32)
        if k == ENTER_AFTER:
            pl.when(jnp.logical_not(at_once))(enter)
    part[...] = total.astype(BF16).reshape(n_red, piece, width)

    @pl.when(core == 1)
    def _():
        pl.semaphore_wait(mate_in, 1)
        m_copy.start()

    p1_copies = {}
    for d in reversed(range(1, n_prow)):
        t = to(d)
        p1_copies[d] = pltpu.make_async_remote_copy(
            part.at[lax.rem(t, n_red)], got.at[d], p1_send, p1_recv,
            device_id=(t, col), device_id_type=MESH)
        pl.when(is_red(t) & lower(d))(p1_copies[d].start)

    inv_load.wait()
    pv_row = pv_ref[...].astype(F32)
    previous, via, chain, landing = swap_plan(pv_row, column_of(pv_row))

    @pl.when(me < n_red - 1)
    def _():
        pl.semaphore_wait(owner_up, n_red - 1 - me)

    o1_copies = [
        pltpu.make_async_remote_copy(
            a_v.at[pl.ds(t * piece, piece)], origs.at[pl.ds(t * piece, piece)], o1_send, o1_recv,
            device_id=(t, col), device_id_type=MESH)
        for t in range(1, n_red)
    ]
    o_local = pltpu.make_async_copy(a_v.at[pl.ds(0, nb)], origs, o1_recv)

    @pl.when(me == 0)
    def _():
        o_local.start()
        for copy in o1_copies:
            copy.start()

    for d in range(1, n_prow):
        pl.when(is_red(to(d)) & jnp.logical_not(lower(d)))(p1_copies[d].start)

    m_copy.wait_recv()
    l_load.wait()

    @pl.when(core == 1)
    def _():
        for k in range(tail, chunks):
            for d in range(1, n_y):
                if k == last:
                    y_twice[d - 1].start()
                y_copy(d, k, cols(k)).start()

    def f_copy(d, k, at):
        src = l_full.at[y_from(d), :, at]
        if k >= tail:
            src = both(y_from(d) // CORES, k)
        return pltpu.make_async_remote_copy(
            src, src, f_send, f_recv.at[d - 1, k], device_id=(me, mate), device_id_type=MESH)

    def forward(k):
        if k >= chunks:
            return

        def go(at):
            for d in range(1, n_y):
                y_copy(d, k, at).wait_recv()
                if k < last:
                    f_copy(d, k, at).start()

        if last > k >= tail:
            pl.when(core == 1)(lambda: go(cols(k)))
        else:
            sent(k, go)

    own_rows = origs.at[pl.ds(slot * piece, piece)]
    o2_copies, p2_copies = {}, {}
    for d in range(1, n_prow):
        o2_copies[d] = pltpu.make_async_remote_copy(
            own_rows, own_rows, o2_send, o2_recv,
            device_id=(to(d), col), device_id_type=MESH)
        p2_copies[d] = pltpu.make_async_remote_copy(
            mine, tops.at[pl.ds(slot * piece, piece)], p2_send, p2_recv,
            device_id=(to(d), col), device_id_type=MESH)

    def not_first(d, fn):
        pl.when(me + d != n_prow)(fn)

    def send_orig():
        @pl.when(me == 0)
        def _():
            o_local.wait()

        @pl.when(me > 0)
        def _():
            pltpu.make_async_remote_copy(
                a_v.at[pl.ds(0, piece)], own_rows, o1_send, o1_recv,
                device_id=(0, col), device_id_type=MESH).wait_recv()

        pl.semaphore_wait(rest_up, n_prow - n_red)
        for d in range(1, n_prow):
            not_first(d, o2_copies[d].start)

    def arrive(ref, sem):
        pltpu.make_async_copy(ref, ref, sem).wait()

    def gather(ref, sem):
        if_red(me, lambda: arrive(ref.at[pl.ds(0, nb - piece)], sem))
        pl.when(jnp.logical_not(is_red(me)))(lambda: arrive(ref, sem))

    if_red(me, send_orig)
    def reduce_and_send():
        acc = part[slot].astype(F32)
        arrive(got.at[pl.ds(1, n_prow - 1)], p1_recv)
        for d in range(1, n_prow):
            acc = acc + got[d].astype(F32)
        mine[...] = acc.astype(BF16)
        tops[pl.ds(slot * piece, piece), :] = acc.astype(BF16)
        for d in range(1, n_prow):
            pl.when(me + d == n_prow)(p2_copies[d].start)
        for d in range(1, n_prow):
            not_first(d, p2_copies[d].start)

    pl.when((me > 0) & is_red(me))(reduce_and_send)

    step = min(512, rows)
    for start in range(0, rows, step):
        rows_k = pl.ds(start, step)
        here = one_hot(landing == global_rows((step, 1), 0, start))
        here_v[rows_k, :] = here
        hit = jnp.dot(here, jnp.ones((nb, width), BF16), preferred_element_type=F32)
        out_v[rows_k, :] = jnp.where(hit > 0.5, 0.0, a_v[rows_k, :].astype(F32)).astype(BF16)


    pl.when(me == 0)(reduce_and_send)
    for k in range(min(2, tail)):
        forward(k)

    late = range(2, tail)
    far = (core == 1) | (me >= n_prow * 3 // 4)
    for k in late:
        pl.when(far)(functools.partial(forward, k))

    pl.when(me > 0)(lambda: gather(origs, o2_recv))
    orig = origs[...]
    moved = jnp.dot(chain, orig, preferred_element_type=F32).astype(BF16)
    again = jnp.dot(via, orig, preferred_element_type=F32).astype(BF16)
    for start in range(0, rows, step):
        rows_k = pl.ds(start, step)
        landed = jnp.dot(here_v[rows_k, :], moved, preferred_element_type=F32)
        out_v[rows_k, :] = (out_v[rows_k, :].astype(F32) + landed).astype(BF16)

    for k in late:
        pl.when(jnp.logical_not(far))(functools.partial(forward, k))
    if tail < last:
        forward(tail)
    gather(tops, p2_recv)
    top_rows = jnp.where(previous >= 0, again, tops[...])
    u_block = jnp.dot(inv_v[...], top_rows, preferred_element_type=F32).astype(BF16)

    def arrived(k):
        def go(at):
            for d in range(1, n_y):
                f_copy(d, k, at).wait_recv()
        if last > k >= tail:
            pl.when(core == 0)(lambda: go(cols(k)))
        elif k < tail:
            sent(k, go)

    def update(first, end, start=None):
        for k in range(first, end):
            arrived(k)
        start, stop = bounds[first] if start is None else start, bounds[end]
        rows_k = pl.ds(start, stop - start)
        panel = l_full[:, :, rows_k].reshape(nb, stop - start)
        product = lax.dot_general(
            panel, u_block, (((0,), (0,)), ((), ())), preferred_element_type=F32)
        out_v[rows_k, :] = (out_v[rows_k, :].astype(F32) - product).astype(BF16)

    most = max(1, tail - 1)

    @pl.when(me > 0)
    def _():
        update(0, most)

    @pl.when(me == 0)
    def _():
        out_v[pl.ds(0, nb), :] = u_block
        update(0, most, nb)

    u_out[...] = u_block
    for k in range(tail + 1, last):
        forward(k)
    split = min(tail + 1, last)
    if split > most:
        update(most, split)
    for k in range(split, last):
        arrived(k)
    forward(last)

    def drain(pieces):
        while pieces:
            some = min(pieces, rows // piece)
            arrive(out_v.at[pl.ds(0, some * piece)], p1_send)
            pieces -= some

    pl.when(jnp.logical_not(is_red(me)))(lambda: drain(n_red))
    pl.when(is_red(me) & (me > 0))(lambda: drain(n_red - 1 + n_prow - 1 + n_prow - 2))
    pl.when(me == 0)(lambda: drain(2 * (n_red - 1) + 2 * (n_prow - 1)))

    def sent_all(lanes):
        tiles = (lanes * (n_y - 1) + rows) // 128
        full = rows // 128
        while tiles:
            count = next((n for n in range(1, n_pcol + 1) if tiles % n == 0 and tiles // n <= full), 0)
            count, wide = (count, tiles // count) if count else (min(n_pcol, tiles // full), full)
            arrive(l_full.at[pl.ds(0, count), :, pl.ds(0, wide * 128)], y_send)
            tiles -= count * wide

    for skip, here in ((0, me > 0), (nb, me == 0)):
        pl.when(here & (core == 0))(functools.partial(sent_all, 2 * (bounds[tail] - skip)))
        pl.when(here & (core == 1))(functools.partial(sent_all, 2 * (2 * rows - bounds[tail] - skip)))


def last_update(start, in_v, l_full, u_in, out_hbm, end_v, sem):
    rows, width = in_v.shape
    nb = u_in.shape[0]
    rows_k = pl.ds(start, rows - start)
    pltpu.make_async_copy(in_v.at[pl.ds(0, start)], out_hbm.at[pl.ds(0, start)], sem).start()
    panel = l_full[:, :, rows_k].reshape(nb, rows - start)
    product = lax.dot_general(panel, u_in[...], (((0,), (0,)), ((), ())), preferred_element_type=F32)
    end_v[...] = (in_v[rows_k, :].astype(F32) - product).astype(BF16)
    pltpu.make_async_copy(end_v, out_hbm.at[rows_k], sem).start()
    pltpu.make_async_copy(in_v, out_hbm, sem).wait()


def hbm(array):
    return pltpu.with_memory_space_constraint(array, pltpu.HBM)


def chunk_bounds(rows, nb):
    last = min(5 * nb, (rows - nb) // 2)
    bounds = [0, min(5 * nb, rows - last)]
    while bounds[-1] < rows - last:
        bounds.append(min(bounds[-1] + 4 * nb, rows - last))
    tail = len(bounds) - 1
    if last == 5 * nb:
        bounds += [rows - 5 * nb // 2, rows - nb]
    return (*bounds, rows), tail


def body(n_prow, n_pcol, a_matrix, l_panel, l_inverse, pivots):
    rows, width = a_matrix.shape
    nb = l_inverse.shape[0]
    depth = l_panel.shape[1]
    n_red = min(n_prow // 2, nb // 16)
    piece = nb // n_red
    n_y = n_pcol // CORES
    bounds, tail = chunk_bounds(rows, nb)
    chunks = len(bounds) - 1
    dma = pltpu.SemaphoreType.DMA
    flag = pltpu.SemaphoreType.REGULAR
    most_rows, l_all, u_block = pl.pallas_call(
        functools.partial(kernel, n_prow, n_pcol, bounds, tail),
        out_shape=[
            jax.ShapeDtypeStruct((rows, width), BF16),
            jax.ShapeDtypeStruct((n_pcol, depth, rows), BF16),
            jax.ShapeDtypeStruct((nb, width), BF16),
        ],
        in_specs=[pl.BlockSpec(memory_space=pl.ANY)] * 4,
        out_specs=[pl.BlockSpec(memory_space=pltpu.VMEM)] * 3,
        scratch_shapes=[
            pltpu.VMEM((rows, width), BF16),
            pltpu.VMEM((rows, nb), BF16),
            pltpu.VMEM((nb, nb), BF16),
            pltpu.VMEM((1, nb), jnp.int32),
            pltpu.VMEM((n_red, piece, width), BF16),
            pltpu.VMEM((n_prow, piece, width), BF16),
            pltpu.VMEM((piece, width), BF16),
            pltpu.VMEM((nb, width), BF16),
            pltpu.VMEM((nb, width), BF16),
            dma((2,)), dma((LOADS,)), dma((2,)), dma((5,)),
            dma((max(n_y - 1, 1), chunks)), dma((max(n_y - 1, 1), max(chunks - 1, 1))), flag((3,)),
        ],
        compiler_params=pltpu.CompilerParams(
            collective_id=0, has_side_effects=True, vmem_limit_bytes=24 * 2 ** 20),
    )(hbm(a_matrix), hbm(l_panel.T), hbm(l_inverse), hbm(pivots.reshape(1, nb)))
    start = bounds[min(tail + 1, chunks - 1)]
    return pl.pallas_call(
        functools.partial(last_update, start),
        out_shape=jax.ShapeDtypeStruct((rows, width), BF16),
        in_specs=[pl.BlockSpec(memory_space=pltpu.VMEM)] * 3,
        out_specs=pl.BlockSpec(memory_space=pltpu.HBM),
        scratch_shapes=[pltpu.VMEM((rows - start, width), BF16), dma],
        compiler_params=pltpu.CompilerParams(vmem_limit_bytes=8 * 2 ** 20),
    )(most_rows, l_all, u_block)


def solution(mesh):
    n_prow, n_pcol = mesh.shape["prow"], mesh.shape["pcol"]
    in_specs = (P("prow", "pcol"), P("prow", "pcol"), P(), P())
    return jax.shard_map(
        functools.partial(body, n_prow, n_pcol),
        mesh=mesh, in_specs=in_specs, out_specs=P("prow", "pcol"), check_vma=False)
```

```python
import functools

import jax
import jax.numpy as jnp
from jax import lax
from jax.experimental import pallas as pl
from jax.experimental.pallas import tpu as pltpu
from jax.sharding import PartitionSpec as P

MESH = pl.DeviceIdType.MESH
F32 = jnp.float32
BF16 = jnp.bfloat16
CORES = 2
LOADS = 2
ENTER_AFTER = 0


def one_hot(mask):
    return jnp.where(mask, 1.0, 0.0).astype(BF16)


def column_of(pv_row):
    nb = pv_row.shape[1]
    slot = lax.broadcasted_iota(jnp.int32, (nb, nb), 0)
    other = lax.broadcasted_iota(jnp.int32, (nb, nb), 1)
    return jnp.max(jnp.where(slot == other, pv_row, -1.0), axis=1, keepdims=True)


def swap_plan(pv_row, pv_col):
    nb = pv_row.shape[1]
    slot = lax.broadcasted_iota(jnp.int32, (nb, nb), 0).astype(F32)
    other = lax.broadcasted_iota(jnp.int32, (nb, nb), 1).astype(F32)
    slot_col = lax.broadcasted_iota(jnp.int32, (nb, 1), 0).astype(F32)
    earlier = other < slot
    pointer = jnp.max(jnp.where((pv_row == slot) & earlier, other, -1.0), axis=1, keepdims=True)
    chain = one_hot(other == jnp.where(pointer >= 0, pointer, slot_col))
    for _ in range((nb - 1).bit_length()):
        chain = jnp.dot(chain, chain, preferred_element_type=F32).astype(BF16)
    same = pv_row == pv_col
    previous = jnp.max(jnp.where(same & earlier, other, -1.0), axis=1, keepdims=True)
    via = jnp.dot(one_hot(other == previous), chain, preferred_element_type=F32).astype(BF16)
    repeated = jnp.max(jnp.where(same & (slot > other), 1.0, 0.0), axis=0, keepdims=True)
    landing = jnp.where((repeated < 0.5) & (pv_row >= nb), pv_row, -1.0)
    return previous, via, chain, landing


def kernel(
    n_prow, n_pcol, bounds, tail,
    a_hbm, l_hbm, inv_hbm, pv_hbm, out_v, l_full, u_out,
    a_v, here_v, inv_v, pv_ref, part, got, mine, tops, origs,
    load_sem, a_sem, send_sem, recv_sem, y_recv, f_recv, flags,
):
    p1_send = p2_send = o1_send = o2_send = send_sem.at[0]
    y_send = m_send = f_send = send_sem.at[1]
    p1_recv, p2_recv, o1_recv, o2_recv, m_recv = (recv_sem.at[i] for i in range(5))
    owner_up, rest_up, mate_in = (flags.at[i] for i in range(3))
    rows, width = a_v.shape
    nb = inv_v.shape[0]
    n_red, piece, _ = part.shape
    depth = l_full.shape[1]
    n_y = n_pcol // CORES
    chunks = len(bounds) - 1
    me = lax.axis_index("prow")
    col = lax.axis_index("pcol")
    y, core = col // CORES, col % CORES
    mate = y * CORES + (1 - core)

    def y_peer(d):
        return lax.rem(y + d, n_y) * CORES + core

    def y_from(d):
        return lax.rem(y + n_y - d, n_y) * CORES + core

    def to(d):
        return lax.rem(me + d, n_prow)

    def frm(d):
        return lax.rem(me + n_prow - d, n_prow)

    def lower(d):
        return me + d >= n_prow

    def is_red(index):
        return index < n_red

    def if_red(index, fn):
        pl.when(is_red(index))(fn)

    slot = lax.rem(me, n_red)

    barrier = pltpu.get_barrier_semaphore()
    for d in range(1, n_y):
        pl.semaphore_signal(barrier, inc=1, device_id=(me, y_peer(d)), device_id_type=MESH)

    @pl.when(core == 1)
    def _():
        pl.semaphore_signal(barrier, inc=1, device_id=(me, mate), device_id_type=MESH)

    pv_load = pltpu.make_async_copy(pv_hbm, pv_ref, load_sem.at[0])
    pv_load.start()
    block = rows // LOADS
    a_loads = [
        pltpu.make_async_copy(
            a_hbm.at[pl.ds(k * block, block)], a_v.at[pl.ds(k * block, block)], a_sem.at[k])
        for k in range(LOADS)
    ]
    for load in a_loads:
        load.start()
    for d in range(1, n_prow):
        @pl.when(is_red(me) & jnp.logical_not(lower(d)))
        def _():
            pl.semaphore_signal(barrier, inc=1, device_id=(to(d), y * CORES), device_id_type=MESH)

    l_load = pltpu.make_async_copy(l_hbm, l_full.at[col], load_sem.at[1])
    inv_load = pltpu.make_async_copy(inv_hbm, inv_v, load_sem.at[0])

    def cols(k):
        return pl.ds(bounds[k], bounds[k + 1] - bounds[k])

    def sent(k, fn):
        if k == 0:
            pl.when(me > 0)(lambda: fn(cols(k)))
            pl.when(me == 0)(lambda: fn(pl.ds(nb, bounds[1] - nb)))
        else:
            fn(cols(k))

    def both(chip, k):
        return l_full.at[pl.ds(chip * CORES, CORES), :, cols(k)]

    def y_copy(d, k, at):
        src, dst = l_hbm.at[:, at], l_full.at[col, :, at]
        if k >= tail:
            src = dst = both(y, k)
        return pltpu.make_async_remote_copy(
            src, dst, y_send, y_recv.at[d - 1, k], device_id=(me, y_peer(d)), device_id_type=MESH)

    last = chunks - 1
    again_first = last - 1 if last - 1 > tail else last

    def y_twice(d, k):
        return pltpu.make_async_remote_copy(
            both(y, k), both(y, k), y_send, y_recv.at[d - 1, k],
            device_id=(me, y_peer(d) - core), device_id_type=MESH)

    m_copy = pltpu.make_async_remote_copy(
        l_hbm, l_full.at[col], m_send, m_recv, device_id=(me, mate), device_id_type=MESH)

    def enter():
        pl.semaphore_wait(
            barrier, n_y - 1 + jnp.where(core == 0, 1 + CORES * jnp.minimum(me, n_red), 0))
        for k in range(tail):
            for d in range(1, n_y):
                sent(k, lambda at: y_copy(d, k, at).start())
        @pl.when(core == 0)
        def _():
            pl.semaphore_signal(mate_in, inc=1, device_id=(me, mate), device_id_type=MESH)
            m_copy.start()
            for d in range(1, n_prow):
                for c in range(CORES):
                    there = (to(d), y * CORES + c)

                    @pl.when(is_red(me) & lower(d))
                    def _():
                        pl.semaphore_signal(owner_up, inc=1, device_id=there, device_id_type=MESH)

                    @pl.when(jnp.logical_not(is_red(me)) & is_red(to(d)))
                    def _():
                        pl.semaphore_signal(rest_up, inc=1, device_id=there, device_id_type=MESH)

    at_once = (core == 1) | (me == 0)
    pl.when(at_once)(enter)
    l_load.start()

    def global_rows(shape, axis, start):
        local = lax.broadcasted_iota(jnp.int32, shape, axis) + start
        return ((local // nb * n_prow + me) * nb + local % nb).astype(F32)

    pv_load.wait()
    inv_load.start()
    pv_row = pv_ref[...].astype(F32)
    pv_col = column_of(pv_row)
    total = jnp.zeros((nb, width), F32)
    for k in range(LOADS):
        a_loads[k].wait()
        pick = one_hot(pv_col == global_rows((1, block), 1, k * block))
        total = total + jnp.dot(pick, a_v[pl.ds(k * block, block), :], preferred_element_type=F32)
        if k == ENTER_AFTER:
            pl.when(jnp.logical_not(at_once))(enter)
    part[...] = total.astype(BF16).reshape(n_red, piece, width)

    @pl.when(core == 1)
    def _():
        pl.semaphore_wait(mate_in, 1)
        m_copy.start()

    p1_copies = {}
    for d in reversed(range(1, n_prow)):
        t = to(d)
        p1_copies[d] = pltpu.make_async_remote_copy(
            part.at[lax.rem(t, n_red)], got.at[d], p1_send, p1_recv,
            device_id=(t, col), device_id_type=MESH)
        pl.when(is_red(t) & lower(d))(p1_copies[d].start)

    inv_load.wait()
    pv_row = pv_ref[...].astype(F32)
    previous, via, chain, landing = swap_plan(pv_row, column_of(pv_row))

    @pl.when(me < n_red - 1)
    def _():
        pl.semaphore_wait(owner_up, n_red - 1 - me)

    o1_copies = [
        pltpu.make_async_remote_copy(
            a_v.at[pl.ds(t * piece, piece)], origs.at[pl.ds(t * piece, piece)], o1_send, o1_recv,
            device_id=(t, col), device_id_type=MESH)
        for t in range(1, n_red)
    ]
    o_local = pltpu.make_async_copy(a_v.at[pl.ds(0, nb)], origs, o1_recv)

    @pl.when(me == 0)
    def _():
        o_local.start()
        for copy in o1_copies:
            copy.start()

    for d in range(1, n_prow):
        pl.when(is_red(to(d)) & jnp.logical_not(lower(d)))(p1_copies[d].start)

    m_copy.wait_recv()
    l_load.wait()

    @pl.when(core == 1)
    def _():
        for k in range(tail, chunks):
            for d in range(1, n_y):
                if k == again_first:
                    @pl.when(me == 0)
                    def _():
                        for j in range(again_first, chunks):
                            y_twice(d, j).start()
                if k == last:
                    pl.when(me > 0)(lambda: y_twice(d, k).start())
                y_copy(d, k, cols(k)).start()

    def f_copy(d, k, at):
        src = l_full.at[y_from(d), :, at]
        if k >= tail:
            src = both(y_from(d) // CORES, k)
        return pltpu.make_async_remote_copy(
            src, src, f_send, f_recv.at[d - 1, k], device_id=(me, mate), device_id_type=MESH)

    def forward(k):
        if k >= chunks:
            return

        def go(at):
            for d in range(1, n_y):
                y_copy(d, k, at).wait_recv()
                if k == again_first < last:
                    pl.when(me > 0)(lambda: f_copy(d, k, at).start())
                elif k < last:
                    f_copy(d, k, at).start()

        if last > k >= tail:
            pl.when(core == 1)(lambda: go(cols(k)))
        else:
            sent(k, go)

    own_rows = origs.at[pl.ds(slot * piece, piece)]
    o2_copies, p2_copies = {}, {}
    for d in range(1, n_prow):
        o2_copies[d] = pltpu.make_async_remote_copy(
            own_rows, own_rows, o2_send, o2_recv,
            device_id=(to(d), col), device_id_type=MESH)
        p2_copies[d] = pltpu.make_async_remote_copy(
            mine, tops.at[pl.ds(slot * piece, piece)], p2_send, p2_recv,
            device_id=(to(d), col), device_id_type=MESH)

    def not_first(d, fn):
        pl.when(me + d != n_prow)(fn)

    def send_orig():
        @pl.when(me == 0)
        def _():
            o_local.wait()

        @pl.when(me > 0)
        def _():
            pltpu.make_async_remote_copy(
                a_v.at[pl.ds(0, piece)], own_rows, o1_send, o1_recv,
                device_id=(0, col), device_id_type=MESH).wait_recv()

        pl.semaphore_wait(rest_up, n_prow - n_red)
        for d in range(1, n_prow):
            not_first(d, o2_copies[d].start)

    def arrive(ref, sem):
        pltpu.make_async_copy(ref, ref, sem).wait()

    def gather(ref, sem):
        if_red(me, lambda: arrive(ref.at[pl.ds(0, nb - piece)], sem))
        pl.when(jnp.logical_not(is_red(me)))(lambda: arrive(ref, sem))

    if_red(me, send_orig)
    def reduce_and_send():
        acc = part[slot].astype(F32)
        arrive(got.at[pl.ds(1, n_prow - 1)], p1_recv)
        for d in range(1, n_prow):
            acc = acc + got[d].astype(F32)
        mine[...] = acc.astype(BF16)
        tops[pl.ds(slot * piece, piece), :] = acc.astype(BF16)
        for d in range(1, n_prow):
            pl.when(me + d == n_prow)(p2_copies[d].start)
        for d in range(1, n_prow):
            not_first(d, p2_copies[d].start)

    pl.when((me > 0) & is_red(me))(reduce_and_send)

    step = min(512, rows)
    for start in range(0, rows, step):
        rows_k = pl.ds(start, step)
        here = one_hot(landing == global_rows((step, 1), 0, start))
        here_v[rows_k, :] = here
        hit = jnp.dot(here, jnp.ones((nb, width), BF16), preferred_element_type=F32)
        out_v[rows_k, :] = jnp.where(hit > 0.5, 0.0, a_v[rows_k, :].astype(F32)).astype(BF16)


    pl.when(me == 0)(reduce_and_send)
    for k in range(min(2, tail)):
        forward(k)

    late = range(2, tail)
    far = (core == 1) | (me >= n_prow * 3 // 4)
    for k in late:
        pl.when(far)(functools.partial(forward, k))

    pl.when(me > 0)(lambda: gather(origs, o2_recv))
    orig = origs[...]
    moved = jnp.dot(chain, orig, preferred_element_type=F32).astype(BF16)
    again = jnp.dot(via, orig, preferred_element_type=F32).astype(BF16)
    for start in range(0, rows, step):
        rows_k = pl.ds(start, step)
        landed = jnp.dot(here_v[rows_k, :], moved, preferred_element_type=F32)
        out_v[rows_k, :] = (out_v[rows_k, :].astype(F32) + landed).astype(BF16)

    for k in late:
        pl.when(jnp.logical_not(far))(functools.partial(forward, k))
    if tail < last:
        forward(tail)
    gather(tops, p2_recv)
    top_rows = jnp.where(previous >= 0, again, tops[...])
    u_block = jnp.dot(inv_v[...], top_rows, preferred_element_type=F32).astype(BF16)

    def arrived(k):
        def go(at):
            for d in range(1, n_y):
                if k == again_first < last:
                    pl.when(me > 0)(lambda: f_copy(d, k, at).wait_recv())
                    pl.when(me == 0)(lambda: y_copy(d, k, at).wait_recv())
                else:
                    f_copy(d, k, at).wait_recv()
        if last > k >= tail:
            pl.when(core == 0)(lambda: go(cols(k)))
        elif k < tail:
            sent(k, go)

    def update(first, end, start=None):
        for k in range(first, end):
            arrived(k)
        start, stop = bounds[first] if start is None else start, bounds[end]
        rows_k = pl.ds(start, stop - start)
        panel = l_full[:, :, rows_k].reshape(nb, stop - start)
        product = lax.dot_general(
            panel, u_block, (((0,), (0,)), ((), ())), preferred_element_type=F32)
        out_v[rows_k, :] = (out_v[rows_k, :].astype(F32) - product).astype(BF16)

    most = max(1, tail - 1)

    @pl.when(me > 0)
    def _():
        update(0, most)

    @pl.when(me == 0)
    def _():
        out_v[pl.ds(0, nb), :] = u_block
        update(0, most, nb)

    u_out[...] = u_block
    for k in range(tail + 1, last):
        forward(k)
    split = min(tail + 1, last)
    if split > most:
        update(most, split)
    for k in range(split, last):
        arrived(k)
    forward(last)

    def drain(pieces):
        while pieces:
            some = min(pieces, rows // piece)
            arrive(out_v.at[pl.ds(0, some * piece)], p1_send)
            pieces -= some

    pl.when(jnp.logical_not(is_red(me)))(lambda: drain(n_red))
    pl.when(is_red(me) & (me > 0))(lambda: drain(n_red - 1 + n_prow - 1 + n_prow - 2))
    pl.when(me == 0)(lambda: drain(2 * (n_red - 1) + 2 * (n_prow - 1)))

    def sent_all(lanes):
        tiles = (lanes * (n_y - 1) + rows) // 128
        full = rows // 128
        while tiles:
            count = next((n for n in range(1, n_pcol + 1) if tiles % n == 0 and tiles // n <= full), 0)
            count, wide = (count, tiles // count) if count else (min(n_pcol, tiles // full), full)
            arrive(l_full.at[pl.ds(0, count), :, pl.ds(0, wide * 128)], y_send)
            tiles -= count * wide

    for skip, here in ((0, me > 0), (nb, me == 0)):
        pl.when(here & (core == 0))(functools.partial(sent_all, 2 * (bounds[tail] - skip)))
        pl.when(here & (core == 1))(functools.partial(sent_all, 2 * (2 * rows - bounds[tail] - skip)))


def last_update(start, in_v, l_full, u_in, out_hbm, end_v, sem):
    rows, width = in_v.shape
    nb = u_in.shape[0]
    rows_k = pl.ds(start, rows - start)
    pltpu.make_async_copy(in_v.at[pl.ds(0, start)], out_hbm.at[pl.ds(0, start)], sem).start()
    panel = l_full[:, :, rows_k].reshape(nb, rows - start)
    product = lax.dot_general(panel, u_in[...], (((0,), (0,)), ((), ())), preferred_element_type=F32)
    end_v[...] = (in_v[rows_k, :].astype(F32) - product).astype(BF16)
    pltpu.make_async_copy(end_v, out_hbm.at[rows_k], sem).start()
    pltpu.make_async_copy(in_v, out_hbm, sem).wait()


def hbm(array):
    return pltpu.with_memory_space_constraint(array, pltpu.HBM)


def chunk_bounds(rows, nb):
    last = min(5 * nb, (rows - nb) // 2)
    bounds = [0, min(5 * nb, rows - last)]
    while bounds[-1] < rows - last:
        bounds.append(min(bounds[-1] + 4 * nb, rows - last))
    tail = len(bounds) - 1
    if last == 5 * nb:
        bounds += [rows - 5 * nb // 2, rows - nb, rows - nb // 2]
    return (*bounds, rows), tail


def body(n_prow, n_pcol, a_matrix, l_panel, l_inverse, pivots):
    rows, width = a_matrix.shape
    nb = l_inverse.shape[0]
    depth = l_panel.shape[1]
    n_red = min(n_prow // 2, nb // 16)
    piece = nb // n_red
    n_y = n_pcol // CORES
    bounds, tail = chunk_bounds(rows, nb)
    chunks = len(bounds) - 1
    dma = pltpu.SemaphoreType.DMA
    flag = pltpu.SemaphoreType.REGULAR
    most_rows, l_all, u_block = pl.pallas_call(
        functools.partial(kernel, n_prow, n_pcol, bounds, tail),
        out_shape=[
            jax.ShapeDtypeStruct((rows, width), BF16),
            jax.ShapeDtypeStruct((n_pcol, depth, rows), BF16),
            jax.ShapeDtypeStruct((nb, width), BF16),
        ],
        in_specs=[pl.BlockSpec(memory_space=pl.ANY)] * 4,
        out_specs=[pl.BlockSpec(memory_space=pltpu.VMEM)] * 3,
        scratch_shapes=[
            pltpu.VMEM((rows, width), BF16),
            pltpu.VMEM((rows, nb), BF16),
            pltpu.VMEM((nb, nb), BF16),
            pltpu.VMEM((1, nb), jnp.int32),
            pltpu.VMEM((n_red, piece, width), BF16),
            pltpu.VMEM((n_prow, piece, width), BF16),
            pltpu.VMEM((piece, width), BF16),
            pltpu.VMEM((nb, width), BF16),
            pltpu.VMEM((nb, width), BF16),
            dma((2,)), dma((LOADS,)), dma((2,)), dma((5,)),
            dma((max(n_y - 1, 1), chunks)), dma((max(n_y - 1, 1), max(chunks - 1, 1))), flag((3,)),
        ],
        compiler_params=pltpu.CompilerParams(
            collective_id=0, has_side_effects=True, vmem_limit_bytes=24 * 2 ** 20),
    )(hbm(a_matrix), hbm(l_panel.T), hbm(l_inverse), hbm(pivots.reshape(1, nb)))
    start = bounds[min(tail + 1, chunks - 1)]
    return pl.pallas_call(
        functools.partial(last_update, start),
        out_shape=jax.ShapeDtypeStruct((rows, width), BF16),
        in_specs=[pl.BlockSpec(memory_space=pltpu.VMEM)] * 3,
        out_specs=pl.BlockSpec(memory_space=pltpu.HBM),
        scratch_shapes=[pltpu.VMEM((rows - start, width), BF16), dma],
        compiler_params=pltpu.CompilerParams(vmem_limit_bytes=8 * 2 ** 20),
    )(most_rows, l_all, u_block)


def solution(mesh):
    n_prow, n_pcol = mesh.shape["prow"], mesh.shape["pcol"]
    in_specs = (P("prow", "pcol"), P("prow", "pcol"), P(), P())
    return jax.shard_map(
        functools.partial(body, n_prow, n_pcol),
        mesh=mesh, in_specs=in_specs, out_specs=P("prow", "pcol"), check_vma=False)
```

```python
import functools

import jax
import jax.numpy as jnp
from jax import lax
from jax.experimental import pallas as pl
from jax.experimental.pallas import tpu as pltpu
from jax.sharding import PartitionSpec as P

MESH = pl.DeviceIdType.MESH
F32 = jnp.float32
BF16 = jnp.bfloat16
CORES = 2
LOADS = 2
ENTER_AFTER = 0


def one_hot(mask):
    return jnp.where(mask, 1.0, 0.0).astype(BF16)


def column_of(pv_row):
    nb = pv_row.shape[1]
    slot = lax.broadcasted_iota(jnp.int32, (nb, nb), 0)
    other = lax.broadcasted_iota(jnp.int32, (nb, nb), 1)
    return jnp.max(jnp.where(slot == other, pv_row, -1.0), axis=1, keepdims=True)


def swap_plan(pv_row, pv_col):
    nb = pv_row.shape[1]
    slot = lax.broadcasted_iota(jnp.int32, (nb, nb), 0).astype(F32)
    other = lax.broadcasted_iota(jnp.int32, (nb, nb), 1).astype(F32)
    slot_col = lax.broadcasted_iota(jnp.int32, (nb, 1), 0).astype(F32)
    earlier = other < slot
    pointer = jnp.max(jnp.where((pv_row == slot) & earlier, other, -1.0), axis=1, keepdims=True)
    chain = one_hot(other == jnp.where(pointer >= 0, pointer, slot_col))
    for _ in range((nb - 1).bit_length()):
        chain = jnp.dot(chain, chain, preferred_element_type=F32).astype(BF16)
    same = pv_row == pv_col
    previous = jnp.max(jnp.where(same & earlier, other, -1.0), axis=1, keepdims=True)
    via = jnp.dot(one_hot(other == previous), chain, preferred_element_type=F32).astype(BF16)
    repeated = jnp.max(jnp.where(same & (slot > other), 1.0, 0.0), axis=0, keepdims=True)
    landing = jnp.where((repeated < 0.5) & (pv_row >= nb), pv_row, -1.0)
    return previous, via, chain, landing


def kernel(
    n_prow, n_pcol, bounds, tail,
    a_hbm, l_hbm, inv_hbm, pv_hbm, out_v, l_full, u_out,
    a_v, here_v, inv_v, pv_ref, part, got, mine, tops, origs,
    load_sem, a_sem, send_sem, recv_sem, y_recv, f_recv, flags,
):
    p1_send = p2_send = o1_send = o2_send = send_sem.at[0]
    y_send = m_send = f_send = send_sem.at[1]
    p1_recv, p2_recv, o1_recv, o2_recv, m_recv = (recv_sem.at[i] for i in range(5))
    owner_up, rest_up, mate_in = (flags.at[i] for i in range(3))
    rows, width = a_v.shape
    nb = inv_v.shape[0]
    n_red, piece, _ = part.shape
    depth = l_full.shape[1]
    n_y = n_pcol // CORES
    chunks = len(bounds) - 1
    me = lax.axis_index("prow")
    col = lax.axis_index("pcol")
    y, core = col // CORES, col % CORES
    mate = y * CORES + (1 - core)

    def y_peer(d):
        return lax.rem(y + d, n_y) * CORES + core

    def y_from(d):
        return lax.rem(y + n_y - d, n_y) * CORES + core

    def to(d):
        return lax.rem(me + d, n_prow)

    def frm(d):
        return lax.rem(me + n_prow - d, n_prow)

    def lower(d):
        return me + d >= n_prow

    def is_red(index):
        return index < n_red

    def if_red(index, fn):
        pl.when(is_red(index))(fn)

    slot = lax.rem(me, n_red)

    barrier = pltpu.get_barrier_semaphore()
    for d in range(1, n_y):
        pl.semaphore_signal(barrier, inc=1, device_id=(me, y_peer(d)), device_id_type=MESH)

    @pl.when(core == 1)
    def _():
        pl.semaphore_signal(barrier, inc=1, device_id=(me, mate), device_id_type=MESH)

    pv_load = pltpu.make_async_copy(pv_hbm, pv_ref, load_sem.at[0])
    pv_load.start()
    block = rows // LOADS
    a_loads = [
        pltpu.make_async_copy(
            a_hbm.at[pl.ds(k * block, block)], a_v.at[pl.ds(k * block, block)], a_sem.at[k])
        for k in range(LOADS)
    ]
    for load in a_loads:
        load.start()
    for d in range(1, n_prow):
        @pl.when(is_red(me) & jnp.logical_not(lower(d)))
        def _():
            pl.semaphore_signal(barrier, inc=1, device_id=(to(d), y * CORES), device_id_type=MESH)

    l_load = pltpu.make_async_copy(l_hbm, l_full.at[col], load_sem.at[1])
    inv_load = pltpu.make_async_copy(inv_hbm, inv_v, load_sem.at[0])

    def cols(k):
        return pl.ds(bounds[k], bounds[k + 1] - bounds[k])

    def sent(k, fn):
        if k == 0:
            pl.when(me > 0)(lambda: fn(cols(k)))
            pl.when(me == 0)(lambda: fn(pl.ds(nb, bounds[1] - nb)))
        else:
            fn(cols(k))

    def both(chip, k):
        return l_full.at[pl.ds(chip * CORES, CORES), :, cols(k)]

    def y_copy(d, k, at):
        src, dst = l_hbm.at[:, at], l_full.at[col, :, at]
        if k >= tail:
            src = dst = both(y, k)
        return pltpu.make_async_remote_copy(
            src, dst, y_send, y_recv.at[d - 1, k], device_id=(me, y_peer(d)), device_id_type=MESH)

    last = chunks - 1
    again_first = last - 1 if last - 1 > tail else last

    def y_twice(d, k):
        return pltpu.make_async_remote_copy(
            both(y, k), both(y, k), y_send, y_recv.at[d - 1, k],
            device_id=(me, y_peer(d) - core), device_id_type=MESH)

    m_copy = pltpu.make_async_remote_copy(
        l_hbm, l_full.at[col], m_send, m_recv, device_id=(me, mate), device_id_type=MESH)

    def enter():
        pl.semaphore_wait(
            barrier, n_y - 1 + jnp.where(core == 0, 1 + CORES * jnp.minimum(me, n_red), 0))
        for k in range(tail):
            for d in range(1, n_y):
                sent(k, lambda at: y_copy(d, k, at).start())
        @pl.when(core == 0)
        def _():
            pl.semaphore_signal(mate_in, inc=1, device_id=(me, mate), device_id_type=MESH)
            m_copy.start()
            for d in range(1, n_prow):
                for c in range(CORES):
                    there = (to(d), y * CORES + c)

                    @pl.when(is_red(me) & lower(d))
                    def _():
                        pl.semaphore_signal(owner_up, inc=1, device_id=there, device_id_type=MESH)

                    @pl.when(jnp.logical_not(is_red(me)) & is_red(to(d)))
                    def _():
                        pl.semaphore_signal(rest_up, inc=1, device_id=there, device_id_type=MESH)

    at_once = (core == 1) | (me == 0)
    pl.when(at_once)(enter)
    l_load.start()

    def global_rows(shape, axis, start):
        local = lax.broadcasted_iota(jnp.int32, shape, axis) + start
        return ((local // nb * n_prow + me) * nb + local % nb).astype(F32)

    pv_load.wait()
    inv_load.start()
    pv_row = pv_ref[...].astype(F32)
    pv_col = column_of(pv_row)
    total = jnp.zeros((nb, width), F32)
    for k in range(LOADS):
        a_loads[k].wait()
        pick = one_hot(pv_col == global_rows((1, block), 1, k * block))
        total = total + jnp.dot(pick, a_v[pl.ds(k * block, block), :], preferred_element_type=F32)
        if k == ENTER_AFTER:
            pl.when(jnp.logical_not(at_once))(enter)
    part[...] = total.astype(BF16).reshape(n_red, piece, width)

    @pl.when(core == 1)
    def _():
        pl.semaphore_wait(mate_in, 1)
        m_copy.start()

    p1_copies = {}
    for d in reversed(range(1, n_prow)):
        t = to(d)
        p1_copies[d] = pltpu.make_async_remote_copy(
            part.at[lax.rem(t, n_red)], got.at[d], p1_send, p1_recv,
            device_id=(t, col), device_id_type=MESH)
        pl.when(is_red(t) & lower(d))(p1_copies[d].start)

    inv_load.wait()
    pv_row = pv_ref[...].astype(F32)
    previous, via, chain, landing = swap_plan(pv_row, column_of(pv_row))

    @pl.when(me < n_red - 1)
    def _():
        pl.semaphore_wait(owner_up, n_red - 1 - me)

    o1_copies = [
        pltpu.make_async_remote_copy(
            a_v.at[pl.ds(t * piece, piece)], origs.at[pl.ds(t * piece, piece)], o1_send, o1_recv,
            device_id=(t, col), device_id_type=MESH)
        for t in range(1, n_red)
    ]
    o_local = pltpu.make_async_copy(a_v.at[pl.ds(0, nb)], origs, o1_recv)

    @pl.when(me == 0)
    def _():
        o_local.start()
        for copy in o1_copies:
            copy.start()

    for d in range(1, n_prow):
        pl.when(is_red(to(d)) & jnp.logical_not(lower(d)))(p1_copies[d].start)

    m_copy.wait_recv()
    l_load.wait()

    @pl.when(core == 1)
    def _():
        for k in range(tail, chunks):
            for d in range(1, n_y):
                if k == again_first:
                    @pl.when(me == 0)
                    def _():
                        for j in range(again_first, chunks):
                            y_twice(d, j).start()
                if k == last:
                    pl.when(me > 0)(lambda: y_twice(d, k).start())
                y_copy(d, k, cols(k)).start()

    def f_copy(d, k, at):
        src = l_full.at[y_from(d), :, at]
        if k >= tail:
            src = both(y_from(d) // CORES, k)
        return pltpu.make_async_remote_copy(
            src, src, f_send, f_recv.at[d - 1, k], device_id=(me, mate), device_id_type=MESH)

    def forward(k):
        if k >= chunks:
            return

        def go(at):
            for d in range(1, n_y):
                y_copy(d, k, at).wait_recv()
                if k == again_first < last:
                    pl.when(me > 0)(lambda: f_copy(d, k, at).start())
                elif k < last:
                    f_copy(d, k, at).start()

        if last > k >= tail:
            pl.when(core == 1)(lambda: go(cols(k)))
        else:
            sent(k, go)

    own_rows = origs.at[pl.ds(slot * piece, piece)]
    o2_copies, p2_copies = {}, {}
    for d in range(1, n_prow):
        o2_copies[d] = pltpu.make_async_remote_copy(
            own_rows, own_rows, o2_send, o2_recv,
            device_id=(to(d), col), device_id_type=MESH)
        p2_copies[d] = pltpu.make_async_remote_copy(
            mine, tops.at[pl.ds(slot * piece, piece)], p2_send, p2_recv,
            device_id=(to(d), col), device_id_type=MESH)

    def not_first(d, fn):
        pl.when(me + d != n_prow)(fn)

    def send_orig():
        @pl.when(me == 0)
        def _():
            o_local.wait()

        @pl.when(me > 0)
        def _():
            pltpu.make_async_remote_copy(
                a_v.at[pl.ds(0, piece)], own_rows, o1_send, o1_recv,
                device_id=(0, col), device_id_type=MESH).wait_recv()

        pl.semaphore_wait(rest_up, n_prow - n_red)
        for d in reversed(range(1, n_prow)):
            not_first(d, o2_copies[d].start)

    def arrive(ref, sem):
        pltpu.make_async_copy(ref, ref, sem).wait()

    def gather(ref, sem):
        if_red(me, lambda: arrive(ref.at[pl.ds(0, nb - piece)], sem))
        pl.when(jnp.logical_not(is_red(me)))(lambda: arrive(ref, sem))

    if_red(me, send_orig)
    def reduce_and_send():
        acc = part[slot].astype(F32)
        arrive(got.at[pl.ds(1, n_prow - 1)], p1_recv)
        for d in range(1, n_prow):
            acc = acc + got[d].astype(F32)
        mine[...] = acc.astype(BF16)
        tops[pl.ds(slot * piece, piece), :] = acc.astype(BF16)
        for d in range(1, n_prow):
            pl.when(me + d == n_prow)(p2_copies[d].start)
        for d in reversed(range(1, n_prow)):
            not_first(d, p2_copies[d].start)

    pl.when((me > 0) & is_red(me))(reduce_and_send)

    step = min(512, rows)
    for start in range(0, rows, step):
        rows_k = pl.ds(start, step)
        here = one_hot(landing == global_rows((step, 1), 0, start))
        here_v[rows_k, :] = here
        hit = jnp.dot(here, jnp.ones((nb, width), BF16), preferred_element_type=F32)
        out_v[rows_k, :] = jnp.where(hit > 0.5, 0.0, a_v[rows_k, :].astype(F32)).astype(BF16)


    pl.when(me == 0)(reduce_and_send)
    for k in range(min(2, tail)):
        forward(k)

    late = range(2, tail)
    far = (core == 1) | (me >= n_prow // 2)
    for k in late:
        pl.when(far)(functools.partial(forward, k))

    pl.when(me > 0)(lambda: gather(origs, o2_recv))
    orig = origs[...]
    moved = jnp.dot(chain, orig, preferred_element_type=F32).astype(BF16)
    again = jnp.dot(via, orig, preferred_element_type=F32).astype(BF16)
    for start in range(0, rows, step):
        rows_k = pl.ds(start, step)
        landed = jnp.dot(here_v[rows_k, :], moved, preferred_element_type=F32)
        out_v[rows_k, :] = (out_v[rows_k, :].astype(F32) + landed).astype(BF16)

    for k in late:
        pl.when(jnp.logical_not(far))(functools.partial(forward, k))
    if tail < last:
        forward(tail)
    gather(tops, p2_recv)
    top_rows = jnp.where(previous >= 0, again, tops[...])
    u_block = jnp.dot(inv_v[...], top_rows, preferred_element_type=F32).astype(BF16)

    def arrived(k):
        def go(at):
            for d in range(1, n_y):
                if k == again_first < last:
                    pl.when(me > 0)(lambda: f_copy(d, k, at).wait_recv())
                    pl.when(me == 0)(lambda: y_copy(d, k, at).wait_recv())
                else:
                    f_copy(d, k, at).wait_recv()
        if last > k >= tail:
            pl.when(core == 0)(lambda: go(cols(k)))
        elif k < tail:
            sent(k, go)

    def update(first, end, start=None):
        for k in range(first, end):
            arrived(k)
        start, stop = bounds[first] if start is None else start, bounds[end]
        rows_k = pl.ds(start, stop - start)
        panel = l_full[:, :, rows_k].reshape(nb, stop - start)
        product = lax.dot_general(
            panel, u_block, (((0,), (0,)), ((), ())), preferred_element_type=F32)
        out_v[rows_k, :] = (out_v[rows_k, :].astype(F32) - product).astype(BF16)

    most = max(1, tail - 1)

    @pl.when(me > 0)
    def _():
        update(0, most)

    @pl.when(me == 0)
    def _():
        out_v[pl.ds(0, nb), :] = u_block
        update(0, most, nb)

    u_out[...] = u_block
    for k in range(tail + 1, last):
        forward(k)
    split = min(tail + 1, last)
    if split > most:
        update(most, split)
    for k in range(split, last):
        arrived(k)
    forward(last)

    def drain(pieces):
        while pieces:
            some = min(pieces, rows // piece)
            arrive(out_v.at[pl.ds(0, some * piece)], p1_send)
            pieces -= some

    pl.when(jnp.logical_not(is_red(me)))(lambda: drain(n_red))
    pl.when(is_red(me) & (me > 0))(lambda: drain(n_red - 1 + n_prow - 1 + n_prow - 2))
    pl.when(me == 0)(lambda: drain(2 * (n_red - 1) + 2 * (n_prow - 1)))

    def sent_all(lanes):
        tiles = (lanes * (n_y - 1) + rows) // 128
        full = rows // 128
        while tiles:
            count = next((n for n in range(1, n_pcol + 1) if tiles % n == 0 and tiles // n <= full), 0)
            count, wide = (count, tiles // count) if count else (min(n_pcol, tiles // full), full)
            arrive(l_full.at[pl.ds(0, count), :, pl.ds(0, wide * 128)], y_send)
            tiles -= count * wide

    for skip, here in ((0, me > 0), (nb, me == 0)):
        pl.when(here & (core == 0))(functools.partial(sent_all, 2 * (bounds[tail] - skip)))
        pl.when(here & (core == 1))(functools.partial(sent_all, 2 * (2 * rows - bounds[tail] - skip)))


def last_update(start, in_v, l_full, u_in, out_hbm, end_v, sem):
    rows, width = in_v.shape
    nb = u_in.shape[0]
    rows_k = pl.ds(start, rows - start)
    pltpu.make_async_copy(in_v.at[pl.ds(0, start)], out_hbm.at[pl.ds(0, start)], sem).start()
    panel = l_full[:, :, rows_k].reshape(nb, rows - start)
    product = lax.dot_general(panel, u_in[...], (((0,), (0,)), ((), ())), preferred_element_type=F32)
    end_v[...] = (in_v[rows_k, :].astype(F32) - product).astype(BF16)
    pltpu.make_async_copy(end_v, out_hbm.at[rows_k], sem).start()
    pltpu.make_async_copy(in_v, out_hbm, sem).wait()


def hbm(array):
    return pltpu.with_memory_space_constraint(array, pltpu.HBM)


def chunk_bounds(rows, nb):
    last = min(5 * nb, (rows - nb) // 2)
    bounds = [0, min(5 * nb, rows - last)]
    while bounds[-1] < rows - last:
        bounds.append(min(bounds[-1] + 4 * nb, rows - last))
    tail = len(bounds) - 1
    if last == 5 * nb:
        bounds += [rows - 5 * nb // 2, rows - nb, rows - nb // 2]
    return (*bounds, rows), tail


def body(n_prow, n_pcol, a_matrix, l_panel, l_inverse, pivots):
    rows, width = a_matrix.shape
    nb = l_inverse.shape[0]
    depth = l_panel.shape[1]
    n_red = min(n_prow // 2, nb // 16)
    piece = nb // n_red
    n_y = n_pcol // CORES
    bounds, tail = chunk_bounds(rows, nb)
    chunks = len(bounds) - 1
    dma = pltpu.SemaphoreType.DMA
    flag = pltpu.SemaphoreType.REGULAR
    most_rows, l_all, u_block = pl.pallas_call(
        functools.partial(kernel, n_prow, n_pcol, bounds, tail),
        out_shape=[
            jax.ShapeDtypeStruct((rows, width), BF16),
            jax.ShapeDtypeStruct((n_pcol, depth, rows), BF16),
            jax.ShapeDtypeStruct((nb, width), BF16),
        ],
        in_specs=[pl.BlockSpec(memory_space=pl.ANY)] * 4,
        out_specs=[pl.BlockSpec(memory_space=pltpu.VMEM)] * 3,
        scratch_shapes=[
            pltpu.VMEM((rows, width), BF16),
            pltpu.VMEM((rows, nb), BF16),
            pltpu.VMEM((nb, nb), BF16),
            pltpu.VMEM((1, nb), jnp.int32),
            pltpu.VMEM((n_red, piece, width), BF16),
            pltpu.VMEM((n_prow, piece, width), BF16),
            pltpu.VMEM((piece, width), BF16),
            pltpu.VMEM((nb, width), BF16),
            pltpu.VMEM((nb, width), BF16),
            dma((2,)), dma((LOADS,)), dma((2,)), dma((5,)),
            dma((max(n_y - 1, 1), chunks)), dma((max(n_y - 1, 1), max(chunks - 1, 1))), flag((3,)),
        ],
        compiler_params=pltpu.CompilerParams(
            collective_id=0, has_side_effects=True, vmem_limit_bytes=24 * 2 ** 20),
    )(hbm(a_matrix), hbm(l_panel.T), hbm(l_inverse), hbm(pivots.reshape(1, nb)))
    start = bounds[min(tail + 1, chunks - 1)]
    return pl.pallas_call(
        functools.partial(last_update, start),
        out_shape=jax.ShapeDtypeStruct((rows, width), BF16),
        in_specs=[pl.BlockSpec(memory_space=pltpu.VMEM)] * 3,
        out_specs=pl.BlockSpec(memory_space=pltpu.HBM),
        scratch_shapes=[pltpu.VMEM((rows - start, width), BF16), dma],
        compiler_params=pltpu.CompilerParams(vmem_limit_bytes=8 * 2 ** 20),
    )(most_rows, l_all, u_block)


def solution(mesh):
    n_prow, n_pcol = mesh.shape["prow"], mesh.shape["pcol"]
    in_specs = (P("prow", "pcol"), P("prow", "pcol"), P(), P())
    return jax.shard_map(
        functools.partial(body, n_prow, n_pcol),
        mesh=mesh, in_specs=in_specs, out_specs=P("prow", "pcol"), check_vma=False)
```
